32 devices in a mesh: grp: 2 (over x), dev: 16 (over z, y, core).
Axes of the slice: x: 2, y: 2, z: 4, core: 2. Of those that a mesh axis runs over, the one named last changes fastest.
Arguments:
- query: bfloat16 [64, 128, 4096], P(('grp', 'dev')), may hold values from -100 to 100
- grad_out: bfloat16 [64, 128, 4096], P(('grp', 'dev')), may hold values from -6 to 6
- branch_kv: bfloat16 [64, 128, 1024], P(('grp', 'dev')), may hold values from -6 to 6
- root_kv: bfloat16 [1024, 1024], P('dev'), may hold values from -24 to 24
- lengths: int32 [64], P(('grp', 'dev')), may hold values from 0 to 128, as said below
- segments: int32 [64], P(('grp', 'dev')), may hold values from 0 to 3
Outputs:
- query_grad: bfloat16 [64, 128, 4096], P(('grp', 'dev'))
- branch_grad: bfloat16 [64, 128, 1024], P(('grp', 'dev'))
- root_grad: float32 [1024, 1024], P('dev')
The draws below stay inside these ranges and needn't reach their ends.
Inputs may be any that keep to these rules, and one draw needn't show every extreme that they name: `lengths`: A slot with length 0 holds no branch. A device's slots with live positions come before its empty slots. Within a group, device d and device d + 16/2 (d < 8) hold exactly 2 slots with live positions together; a quarter of a group's devices hold 2 such slots and a quarter hold none.
All inputs are finite; a program needn't handle non-finite values.
Results may differ from the reference program's by a relative error of at most 0.0069.
Values may be sent and summed in bfloat16 or wider, within the bound.
No kernel may reach another device: no remote copies, remote signals or barrier semaphores. Data moves between devices by JAX's collectives and lax.ppermute only.
A program may use at most 128 MiB of HBM per device.

```python
import jax
import jax.numpy as jnp
from jax import lax

H = 32
KVH = 4
DH = 128
TILE = 128
R = 1024
SEGS = 4
TILES_DEV = 2
TILES = 64
N_GRP = 2
N_DEV = 16


def root_rows(key):
    drawn = jnp.clip(jax.random.normal(jax.random.fold_in(key, 11), (R, 2 * KVH * DH), jnp.float32), -6.0, 6.0)
    return drawn


def draw_root_kv(key, part):
    return root_rows(key).astype(jnp.bfloat16)


def draw_query(key, part):
    drawn = jnp.clip(jax.random.normal(jax.random.fold_in(key, 21), (TILES, TILE, H * DH), jnp.float32), -6.0, 6.0)
    return drawn.astype(jnp.bfloat16)


def draw_lengths(key, part):
    pairs = N_DEV // 2
    group_keys = jax.random.split(jax.random.fold_in(key, 31), N_GRP)

    def pattern(group_key):
        order_key, side_key = jax.random.split(group_key)
        order = jax.random.permutation(order_key, pairs)
        heavy = order < pairs // 2
        side = jax.random.randint(side_key, (pairs,), 0, 2)
        lower = jnp.where(heavy, 2 * side, 1)
        return jnp.concatenate([lower, 2 - lower])
    counts = jax.vmap(pattern)(group_keys).reshape(N_GRP * N_DEV)
    slots = jnp.arange(TILES_DEV)
    drawn = jax.random.randint(jax.random.fold_in(key, 32), (N_GRP * N_DEV, TILES_DEV), TILE // 4, TILE + 1)
    live = slots[None, :] < counts[:, None]
    return jnp.where(live, drawn, 0).reshape(TILES).astype(jnp.int32)


def place_ends(values, stream_key, smallest, top_value):
    dims = values.shape
    spot = [jax.random.randint(jax.random.fold_in(stream_key, axis), (), 0, dims[axis]) for axis in range(len(dims))]
    values = values.at[tuple(spot)].set(smallest)
    longest = dims.index(max(dims))
    spot[longest] = (spot[longest] + 1) % dims[longest]
    return values.at[tuple(spot)].set(top_value)


def steps_of(own_key, extent, pieces, least, high):
    factor_of, own = 1.0, jax.random.fold_in(own_key, 6)
    for axis_at, parts in pieces:
        draws = jnp.exp(jax.random.uniform(jax.random.fold_in(own, axis_at), (parts,), jnp.float32, least / len(pieces), high / len(pieces)))
        factor_of = factor_of * jnp.repeat(draws, extent[axis_at] // parts).reshape([-1 if axis == axis_at else 1 for axis in range(len(extent))])
    return factor_of


def gaussian(own_key, extent, spread, bound, cuts=(), held_as=jnp.bfloat16):
    result = jax.random.normal(own_key, extent, jnp.float32) * spread
    if len(cuts) > 0:
        result = steps_of(own_key, extent, cuts, -0.22, 0.18) * result
    return jnp.clip(result, min=-bound, max=bound).astype(held_as)


def setup_inputs(seed: int = 0) -> dict:
    key_list = jax.random.split(jax.random.key(seed), 7)
    query = draw_query(jax.random.fold_in(key_list[6], 71), 0)
    grad_out = gaussian(key_list[1], (TILES, TILE, H * DH), 1.0, 6.0, ((0, 32),))
    branch_kv = gaussian(key_list[2], (TILES, TILE, 2 * KVH * DH), 1.0, 6.0, ((0, 32),))
    root_kv = draw_root_kv(jax.random.fold_in(key_list[6], 71), 0)
    lengths = draw_lengths(jax.random.fold_in(key_list[6], 71), 0)
    segments = place_ends(jax.random.randint(key_list[5], (TILES,), 0, SEGS), jax.random.fold_in(key_list[5], 1), 0, SEGS - 1).astype(jnp.int32)
    return dict(query=query, grad_out=grad_out, branch_kv=branch_kv, root_kv=root_kv, lengths=lengths, segments=segments)


def tile_grads(query, grad, branch, length, segment, root_keys):
    rows = query.shape[0]
    width = KVH * DH
    groups = H // KVH
    roots = root_keys.shape[0]
    everything = jnp.concatenate([root_keys, branch], axis=0)
    span = roots + rows
    scale = DH ** -0.5
    row_pos = lax.broadcasted_iota(jnp.int32, (rows, span), 0)
    col_pos = lax.broadcasted_iota(jnp.int32, (rows, span), 1)
    visible = jnp.where(col_pos < roots, col_pos < (segment + 1) * (roots // SEGS), col_pos - roots <= row_pos)
    live = lax.broadcasted_iota(jnp.int32, (rows, 1), 0) < length
    grad = jnp.where(live, grad, jnp.zeros_like(grad))
    dq_parts = []
    dk_parts = []
    dv_parts = []
    for head in range(KVH):
        q_head = query[:, head * groups * DH:(head + 1) * groups * DH].reshape(rows, groups, DH).astype(jnp.float32)
        g_head = grad[:, head * groups * DH:(head + 1) * groups * DH].reshape(rows, groups, DH).astype(jnp.float32)
        k_head = everything[:, head * DH:(head + 1) * DH].astype(jnp.float32)
        v_head = everything[:, width + head * DH:width + (head + 1) * DH].astype(jnp.float32)
        scores = jnp.einsum('tgd,ld->gtl', q_head, k_head) * scale
        scores = jnp.where(visible[None], scores, jnp.float32(-1e30))
        peak = jnp.max(scores, axis=-1, keepdims=True)
        weights = jnp.exp(scores - peak)
        weights = weights / jnp.sum(weights, axis=-1, keepdims=True)
        probs = weights.astype(jnp.bfloat16).astype(jnp.float32)
        output = jnp.einsum('gtl,ld->tgd', probs, v_head)
        delta = jnp.sum(g_head * output, axis=-1)
        dv_parts.append(jnp.einsum('gtl,tgd->ld', probs, g_head))
        prob_grad = jnp.einsum('tgd,ld->gtl', g_head, v_head)
        score_grad = (weights * (prob_grad - delta.T[:, :, None]) * scale).astype(jnp.bfloat16).astype(jnp.float32)
        dq_parts.append(jnp.einsum('gtl,ld->tgd', score_grad, k_head).reshape(rows, groups * DH))
        dk_parts.append(jnp.einsum('gtl,tgd->ld', score_grad, q_head))
    dq = jnp.concatenate(dq_parts, axis=1).astype(jnp.bfloat16)
    dkv = jnp.concatenate(dk_parts + dv_parts, axis=1)
    return dq, dkv[roots:].astype(jnp.bfloat16), dkv[:roots]


def reference(query, grad_out, branch_kv, root_kv, lengths, segments):
    def step(total, items):
        q_tile, g_tile, b_tile, length, segment = items

        def work():
            return tile_grads(q_tile, g_tile, b_tile, length, segment, root_kv)

        def skip():
            return (jnp.zeros(q_tile.shape, jnp.bfloat16), jnp.zeros(b_tile.shape, jnp.bfloat16), jnp.zeros(root_kv.shape, jnp.float32))

        dq, dbranch, droot = lax.cond(length > 0, work, skip)
        return total + droot, (dq, dbranch)

    total, (query_grad, branch_grad) = lax.scan(step, jnp.zeros(root_kv.shape, jnp.float32), (query, grad_out, branch_kv, lengths, segments))
    return query_grad, branch_grad, total
```

```python
import functools
import math

import jax
import jax.numpy as jnp
from jax import lax
from jax.experimental import pallas as pl
from jax.experimental.pallas import tpu as pltpu
from jax.sharding import PartitionSpec as P

H = 32
KVH = 4
DH = 128
SEGS = 4
GROUPS = H // KVH
CORES = 2
HEADS = KVH // CORES
CHUNK = 32
NT = (((1,), (1,)), ((), ()))
NN = (((1,), (0,)), ((), ()))
F32 = jnp.float32
BF16 = jnp.bfloat16


def swapped(block, axis, bit):
    route = [(i ^ bit, i) for i in range(lax.axis_size(axis))]
    return lax.ppermute(block, axis, route)


def dot(a, b, dims):
    return lax.dot_general(a, b, dims, preferred_element_type=F32)


def head_kernel(
    offsets,
    tiles,
    info,
    q_own,
    q_far,
    g_own,
    g_far,
    bk_own,
    bk_far,
    bv_own,
    bv_far,
    kv_near,
    kv_next,
    dq_own,
    dq_far,
    db_own,
    db_far,
    keep,
    send,
    keys,
    values,
    keys_t,
    bkeys,
    bvalues,
    bkeys_t,
    s_scr,
    dp_scr,
    dk_acc,
    dv_acc,
    dbk_acc,
    dbv_acc,
    dq_scr,
):
    t = pl.program_id(0)
    me = info[1]
    rr = kv_near.shape[2]
    rows = q_own.shape[1]
    roots = keys.shape[0]
    width = roots // SEGS
    qrows = GROUPS * CHUNK
    scale = DH ** (-0.5)
    sharp = scale * math.log2(math.e)

    def places():
        for side, bit in ((0, 0), (1, 2)):
            for j, off in enumerate(offsets):
                for b0 in range(CORES):
                    rel = b0 + bit + off
                    yield side, j, b0, pl.multiple_of((me ^ rel) * rr, rr)

    @pl.when(t == 0)
    def _():
        for side, j, b0, at in places():
            block = (kv_near, kv_next)[side][j, b0]
            keys[pl.ds(at, rr), :] = block[:, :DH]
            values[pl.ds(at, rr), :] = block[:, DH:]
        dk_acc[...] = jnp.zeros_like(dk_acc)
        dv_acc[...] = jnp.zeros_like(dv_acc)
        for b in range(0, roots, DH):
            keys_t[:, b : b + DH] = keys[b : b + DH, :].T

    own = t < tiles
    length = info[2 + t]
    segment = info[2 + 2 * tiles + t]

    bkeys[...] = jnp.where(own, bk_own[0], bk_far[0])
    bvalues[...] = jnp.where(own, bv_own[0], bv_far[0])
    bkeys_t[...] = bkeys[...].T
    dbk_acc[...] = jnp.zeros_like(dbk_acc)
    dbv_acc[...] = jnp.zeros_like(dbv_acc)
    dq_scr[...] = jnp.zeros_like(dq_scr)

    def fold(x, op):
        return op(x.reshape(x.shape[0] // 8, 8, x.shape[1]), axis=0)

    def chunk(c, segs):
        r0 = pl.multiple_of(c * CHUNK, CHUNK)

        def taken(near, far):
            x = jnp.where(own, near[0, pl.ds(r0, CHUNK), :], far[0, pl.ds(r0, CHUNK), :])
            return x

        def stacked(x):
            return jnp.concatenate([x[:, j * DH : (j + 1) * DH] for j in range(GROUPS)], axis=0)

        q = stacked(taken(q_own, q_far))
        g = stacked(taken(g_own, g_far))
        row = lax.broadcasted_iota(jnp.int32, (qrows, DH), 0) % CHUNK + r0
        g = jnp.where(row < length, g.astype(F32), 0.0).astype(BF16)

        spans = [(b * width, width) for b in range(segs)] + [(roots, rows)]

        def k_of(b):
            return keys[spans[b][0] : spans[b][0] + width, :] if b < segs else bkeys[...]

        def v_of(b):
            return values[spans[b][0] : spans[b][0] + width, :] if b < segs else bvalues[...]

        def kt_of(b):
            return keys_t[:, spans[b][0] : spans[b][0] + width] if b < segs else bkeys_t[...]

        top = None
        for b in range(segs + 1):
            s = dot(k_of(b), q, NT)
            if b == segs:
                key = lax.broadcasted_iota(jnp.int32, s.shape, 0)
                pos = lax.broadcasted_iota(jnp.int32, s.shape, 1) % CHUNK + r0
                s = jnp.where(key <= pos, s, F32(-1e30))
            s_scr[spans[b][0] : spans[b][0] + spans[b][1], :] = s
            part = fold(s, jnp.max)
            top = part if top is None else jnp.maximum(top, part)
        peak = jnp.max(top, axis=0, keepdims=True)

        total = jnp.zeros((8, qrows), F32)
        for b in range(segs + 1):
            at = slice(spans[b][0], spans[b][0] + spans[b][1])
            dp_scr[at, :] = dot(v_of(b), g, NT)
            e = jnp.exp2((s_scr[at, :] - peak) * sharp)
            s_scr[at, :] = e
            total = total + fold(e, jnp.sum)
        inv = 1.0 / jnp.sum(total, axis=0, keepdims=True)

        delta = jnp.zeros((8, qrows), F32)
        for b in range(segs + 1):
            at = slice(spans[b][0], spans[b][0] + spans[b][1])
            probs = (s_scr[at, :] * inv).astype(BF16)
            delta = delta + fold(probs.astype(F32) * dp_scr[at, :], jnp.sum)
            dv = dot(probs, g, NN)
            if b < segs:
                dv_acc[at, :] += dv
            else:
                dbv_acc[...] += dv
        delta = jnp.sum(delta, axis=0, keepdims=True)
        invs = inv * scale

        dq_t = jnp.zeros((DH, qrows), F32)
        for b in range(segs + 1):
            at = slice(spans[b][0], spans[b][0] + spans[b][1])
            ds = ((s_scr[at, :] * invs) * (dp_scr[at, :] - delta)).astype(BF16)
            dk = dot(ds, q, NN)
            if b < segs:
                dk_acc[at, :] += dk
            else:
                dbk_acc[...] += dk
            dq_t = dq_t + dot(kt_of(b), ds, NN)
        dq = dq_t.T.astype(BF16)
        for j in range(GROUPS):
            dq_scr[pl.ds(r0, CHUNK), j * DH : (j + 1) * DH] = dq[j * CHUNK : (j + 1) * CHUNK, :]

    count = (length + (CHUNK - 1)) // CHUNK
    for s in range(SEGS):

        @pl.when(segment == s)
        def _():
            def step(c, carry):
                chunk(c, s + 1)
                return carry

            lax.fori_loop(0, count, step, 0)

    for mine, dq_ref, db_ref in ((own, dq_own, db_own), (jnp.logical_not(own), dq_far, db_far)):

        @pl.when(mine)
        def _():
            dq_ref[0] = dq_scr[...]
            db_ref[0, :, :DH] = dbk_acc[...].astype(BF16)
            db_ref[0, :, DH:] = dbv_acc[...].astype(BF16)

    @pl.when(t == 2 * tiles - 1)
    def _():
        for side, j, b0, at in places():
            out = (keep, send)[side]
            out[j, b0, :, :DH] = dk_acc[pl.ds(at, rr), :].astype(out.dtype)
            out[j, b0, :, DH:] = dv_acc[pl.ds(at, rr), :].astype(out.dtype)


def head_grads(head, offsets, info, q, q_far, g, g_far, b, b_far, near, nxt):
    tiles, rows, _ = q.shape
    half = near.shape[0]
    rr = near.shape[2]
    roots = 2 * half * CORES * rr
    qw = GROUPS * DH
    qrows = GROUPS * CHUNK

    def low(t):
        return jnp.minimum(t, tiles - 1)

    def high(t):
        return jnp.maximum(t - tiles, 0)

    def col(info):
        return info[0] * HEADS + head

    whole = pl.BlockSpec(near.shape, lambda t, info: (0, 0, 0, 0))
    q_near_spec = pl.BlockSpec((1, rows, qw), lambda t, info: (low(t), 0, col(info)))
    q_far_spec = pl.BlockSpec((1, rows, qw), lambda t, info: (high(t), 0, head))
    in_specs = [
        q_near_spec,
        q_far_spec,
        q_near_spec,
        q_far_spec,
        pl.BlockSpec((1, rows, DH), lambda t, info: (low(t), 0, col(info))),
        pl.BlockSpec((1, rows, DH), lambda t, info: (high(t), 0, head)),
        pl.BlockSpec((1, rows, DH), lambda t, info: (low(t), 0, KVH + col(info))),
        pl.BlockSpec((1, rows, DH), lambda t, info: (high(t), 0, HEADS + head)),
        whole,
        whole,
    ]
    out_specs = [
        pl.BlockSpec((1, rows, qw), lambda t, info: (low(t), 0, 0)),
        pl.BlockSpec((1, rows, qw), lambda t, info: (high(t), 0, 0)),
        pl.BlockSpec((1, rows, 2 * DH), lambda t, info: (low(t), 0, 0)),
        pl.BlockSpec((1, rows, 2 * DH), lambda t, info: (high(t), 0, 0)),
        whole,
        whole,
    ]
    out_shape = [
        jax.ShapeDtypeStruct((tiles, rows, qw), BF16),
        jax.ShapeDtypeStruct((tiles, rows, qw), BF16),
        jax.ShapeDtypeStruct((tiles, rows, 2 * DH), BF16),
        jax.ShapeDtypeStruct((tiles, rows, 2 * DH), BF16),
        jax.ShapeDtypeStruct(near.shape, F32),
        jax.ShapeDtypeStruct(near.shape, BF16),
    ]
    span = roots + rows
    scratch = [
        pltpu.VMEM((roots, DH), BF16),
        pltpu.VMEM((roots, DH), BF16),
        pltpu.VMEM((DH, roots), BF16),
        pltpu.VMEM((rows, DH), BF16),
        pltpu.VMEM((rows, DH), BF16),
        pltpu.VMEM((DH, rows), BF16),
        pltpu.VMEM((span, qrows), F32),
        pltpu.VMEM((span, qrows), F32),
        pltpu.VMEM((roots, DH), F32),
        pltpu.VMEM((roots, DH), F32),
        pltpu.VMEM((rows, DH), F32),
        pltpu.VMEM((rows, DH), F32),
        pltpu.VMEM((rows, qw), BF16),
    ]
    flops = 2 * 5 * tiles * rows * GROUPS * span * DH
    return pl.pallas_call(
        functools.partial(head_kernel, offsets, tiles),
        grid_spec=pltpu.PrefetchScalarGridSpec(
            num_scalar_prefetch=1,
            grid=(2 * tiles,),
            in_specs=in_specs,
            out_specs=out_specs,
            scratch_shapes=scratch,
        ),
        out_shape=out_shape,
        cost_estimate=pl.CostEstimate(
            flops=flops, bytes_accessed=8 * tiles * rows * qw, transcendentals=0
        ),
        compiler_params=pltpu.CompilerParams(dimension_semantics=("arbitrary",)),
        name=f"grads_{head}",
    )(info, q, q_far, g, g_far, b, b_far, b, b_far, near, nxt)


def local(query, grad_out, branch_kv, root_kv, lengths, segments):
    n_dev = lax.axis_size("dev")
    n_grp = lax.axis_size("grp")
    me = lax.axis_index("dev")
    core = me % CORES
    tiles, rows, _ = query.shape
    rr = root_kv.shape[0]
    bits = []
    while (4 << len(bits)) < n_dev:
        bits.append(4 << len(bits))

    def halves(x, parts):
        x = x.reshape(x.shape[:-1] + (parts, CORES, x.shape[-1] // (parts * CORES)))
        axis = x.ndim - 2
        mine = lax.dynamic_index_in_dim(x, core, axis, keepdims=False)
        other = lax.dynamic_index_in_dim(x, 1 - core, axis, keepdims=False)
        flat = x.shape[:-3] + (-1,)
        return mine.reshape(flat), other.reshape(flat)

    mine, other = halves(root_kv, 2)
    block = jnp.stack([mine, swapped(other, "dev", 1)])
    block = block.reshape(1, CORES, rr, 2, HEADS, DH)
    gathered = []
    for head in range(HEADS):
        x = block[:, :, :, :, head, :].reshape(1, CORES, rr, 2 * DH)
        for bit in reversed(bits):
            x = jnp.concatenate([x, swapped(x, "dev", bit)], axis=0)
        gathered.append((x, swapped(x, "dev", 2)))
    offsets = [0]
    for bit in reversed(bits):
        offsets = offsets + [off + bit for off in offsets]

    q_far = swapped(halves(query, 1)[1], "dev", 1)
    g_far = swapped(halves(grad_out, 1)[1], "dev", 1)
    b_far = swapped(halves(branch_kv, 2)[1], "dev", 1)
    meta = jnp.concatenate([lengths, segments]).reshape(2, tiles)
    meta_far = swapped(meta, "dev", 1)
    info = jnp.concatenate(
        [jnp.stack([core, me]), jnp.concatenate([meta, meta_far], axis=1).reshape(-1)]
    )

    q_parts, b_parts, root_parts = [], [], []
    for head in range(HEADS):
        near, nxt = gathered[head]
        dq_own, dq_far, db_own, db_far, keep, send = head_grads(
            head, tuple(offsets), info, query, q_far, grad_out, g_far, branch_kv, b_far, near, nxt
        )
        x = keep + swapped(send, "dev", 2)
        for bit in bits:
            half = x.shape[0] // 2
            x = x[:half] + swapped(x[half:].astype(BF16), "dev", bit)
        x = x[0]
        hop = 1
        while hop < n_grp:
            x = x.astype(BF16)
            x = x.astype(F32) + swapped(x, "grp", hop).astype(F32)
            hop *= 2
        root_parts.append((x[0], swapped(x[1], "dev", 1)))
        q_parts.append((dq_own, swapped(dq_far, "dev", 1)))
        b_parts.append((db_own, swapped(db_far, "dev", 1)))

    def joined(parts, kinds):
        def laid(side):
            x = jnp.stack([p[side].reshape(p[side].shape[:-1] + (kinds, -1)) for p in parts], -2)
            return x.reshape(x.shape[:-2] + (-1,))

        near, far = laid(0), laid(1)
        first = jnp.where(core == 0, near, far)
        second = jnp.where(core == 0, far, near)
        x = jnp.stack([first, second], axis=-2)
        return x.reshape(x.shape[:-3] + (-1,))

    return (joined(q_parts, 1), joined(b_parts, 2), joined(root_parts, 2))


def solution(mesh):
    placed = (
        P(("grp", "dev"), None, None),
        P(("grp", "dev"), None, None),
        P(("grp", "dev"), None, None),
        P("dev", None),
        P(("grp", "dev")),
        P(("grp", "dev")),
    )
    return jax.shard_map(
        local,
        mesh=mesh,
        in_specs=placed,
        out_specs=(P(("grp", "dev"), None, None), P(("grp", "dev"), None, None), P("dev", None)),
        check_vma=False,
    )
```

```python
import functools
import math

import jax
import jax.numpy as jnp
from jax import lax
from jax.experimental import pallas as pl
from jax.experimental.pallas import tpu as pltpu
from jax.sharding import PartitionSpec as P


H = 32
KVH = 4
DH = 128
SEGS = 4
GROUPS = H // KVH
CORES = 2
HEADS = KVH // CORES
CHUNK = 32
NT = (((1,), (1,)), ((), ()))
NN = (((1,), (0,)), ((), ()))
F32 = jnp.float32
BF16 = jnp.bfloat16


def swapped(block, axis, bit):
    route = [(i ^ bit, i) for i in range(lax.axis_size(axis))]
    return lax.ppermute(block, axis, route)


def dot(a, b, dims):
    return lax.dot_general(a, b, dims, preferred_element_type=F32)


def head_kernel(head, offsets, tiles, info, *refs):
    ins, refs = refs[:-19], refs[-19:]
    q_own, q_far, g_own, g_far, bk_own, bk_far, bv_own, bv_far, kv_near, kv_next = ins[:10]
    dq_own, dq_far, db_own, db_far, keep, send = refs[:6]
    keys, values, keys_t, bkeys, bvalues, bkeys_t, s_scr, dp_scr = refs[6:14]
    dk_acc, dv_acc, dbk_acc, dbv_acc, dq_scr = refs[14:]
    t = pl.program_id(0)
    me = info[1]
    rr = kv_near.shape[2]
    rows = q_own.shape[1]
    roots = keys.shape[0]
    width = roots // SEGS
    qrows = GROUPS * CHUNK
    scale = DH ** (-0.5)
    sharp = scale * math.log2(math.e)

    def places():
        for side, bit in ((0, 0), (1, 2)):
            for j, off in enumerate(offsets):
                for b0 in range(CORES):
                    rel = b0 + bit + off
                    yield side, j, b0, pl.multiple_of((me ^ rel) * rr, rr)

    @pl.when(t == 0)
    def _():
        for side, j, b0, at in places():
            block = (kv_near, kv_next)[side][j, b0]
            keys[pl.ds(at, rr), :] = block[:, :DH]
            values[pl.ds(at, rr), :] = block[:, DH:]
        dk_acc[...] = jnp.zeros_like(dk_acc)
        dv_acc[...] = jnp.zeros_like(dv_acc)
        for b in range(0, roots, DH):
            keys_t[:, b : b + DH] = keys[b : b + DH, :].T

    own = t < tiles
    length = info[2 + t]
    segment = info[2 + 2 * tiles + t]

    bkeys[...] = jnp.where(own, bk_own[0], bk_far[0])
    bvalues[...] = jnp.where(own, bv_own[0], bv_far[0])
    bkeys_t[...] = bkeys[...].T
    dbk_acc[...] = jnp.zeros_like(dbk_acc)
    dbv_acc[...] = jnp.zeros_like(dbv_acc)
    dq_scr[...] = jnp.zeros_like(dq_scr)

    def fold(x, op):
        return op(x.reshape(x.shape[0] // 8, 8, x.shape[1]), axis=0)

    def chunk(c, segs):
        r0 = pl.multiple_of(c * CHUNK, CHUNK)

        def taken(near, far):
            x = jnp.where(own, near[0, pl.ds(r0, CHUNK), :], far[0, pl.ds(r0, CHUNK), :])
            return x

        def stacked(x):
            return jnp.concatenate([x[:, j * DH : (j + 1) * DH] for j in range(GROUPS)], axis=0)

        q = stacked(taken(q_own, q_far))
        g = stacked(taken(g_own, g_far))
        row = lax.broadcasted_iota(jnp.int32, (qrows, DH), 0) % CHUNK + r0
        g = jnp.where(row < length, g.astype(F32), 0.0).astype(BF16)

        spans = [(b * width, width) for b in range(segs)] + [(roots, rows)]

        def k_of(b):
            return keys[spans[b][0] : spans[b][0] + width, :] if b < segs else bkeys[...]

        def v_of(b):
            return values[spans[b][0] : spans[b][0] + width, :] if b < segs else bvalues[...]

        def kt_of(b):
            return keys_t[:, spans[b][0] : spans[b][0] + width] if b < segs else bkeys_t[...]

        top = None
        for b in range(segs + 1):
            s = dot(k_of(b), q, NT)
            if b == segs:
                key = lax.broadcasted_iota(jnp.int32, s.shape, 0)
                pos = lax.broadcasted_iota(jnp.int32, s.shape, 1) % CHUNK + r0
                s = jnp.where(key <= pos, s, F32(-1e30))
            s_scr[spans[b][0] : spans[b][0] + spans[b][1], :] = s
            part = fold(s, jnp.max)
            top = part if top is None else jnp.maximum(top, part)
        peak = jnp.max(top, axis=0, keepdims=True)

        total = jnp.zeros((8, qrows), F32)
        for b in range(segs + 1):
            at = slice(spans[b][0], spans[b][0] + spans[b][1])
            dp_scr[at, :] = dot(v_of(b), g, NT)
            e = jnp.exp2((s_scr[at, :] - peak) * sharp)
            s_scr[at, :] = e
            total = total + fold(e, jnp.sum)
        inv = 1.0 / jnp.sum(total, axis=0, keepdims=True)

        delta = jnp.zeros((8, qrows), F32)
        for b in range(segs + 1):
            at = slice(spans[b][0], spans[b][0] + spans[b][1])
            probs = (s_scr[at, :] * inv).astype(BF16)
            delta = delta + fold(probs.astype(F32) * dp_scr[at, :], jnp.sum)
            dv = dot(probs, g, NN)
            if b < segs:
                dv_acc[at, :] += dv
            else:
                dbv_acc[...] += dv
        delta = jnp.sum(delta, axis=0, keepdims=True)
        invs = inv * scale

        dq_t = jnp.zeros((DH, qrows), F32)
        for b in range(segs + 1):
            at = slice(spans[b][0], spans[b][0] + spans[b][1])
            ds = ((s_scr[at, :] * invs) * (dp_scr[at, :] - delta)).astype(BF16)
            dk = dot(ds, q, NN)
            if b < segs:
                dk_acc[at, :] += dk
            else:
                dbk_acc[...] += dk
            dq_t = dq_t + dot(kt_of(b), ds, NN)
        dq = dq_t.T.astype(BF16)
        for j in range(GROUPS):
            dq_scr[pl.ds(r0, CHUNK), j * DH : (j + 1) * DH] = dq[j * CHUNK : (j + 1) * CHUNK, :]

    count = (length + (CHUNK - 1)) // CHUNK
    for s in range(SEGS):

        @pl.when(segment == s)
        def _():
            def step(c, carry):
                chunk(c, s + 1)
                return carry

            lax.fori_loop(0, count, step, 0)

    for side, (mine, dq_ref, db_ref) in enumerate(
        ((own, dq_own, db_own), (jnp.logical_not(own), dq_far, db_far))
    ):

        @pl.when(mine)
        def _():
            dq_ref[0] = dq_scr[...]
            if len(ins) > 10:
                db_ref[0] = ins[12 + side][0]
            at = pl.multiple_of((info[0] * HEADS + head) * DH, DH)
            db_ref[0, :, pl.ds(at, DH)] = dbk_acc[...].astype(BF16)
            db_ref[0, :, pl.ds(at + KVH * DH, DH)] = dbv_acc[...].astype(BF16)

    @pl.when(t == 2 * tiles - 1)
    def _():
        for side, j, b0, at in places():
            out = (keep, send)[side]
            out[j, b0, :, :DH] = dk_acc[pl.ds(at, rr), :].astype(out.dtype)
            out[j, b0, :, DH:] = dv_acc[pl.ds(at, rr), :].astype(out.dtype)


def head_grads(head, offsets, info, q, q_far, g, g_far, b, b_far, near, nxt, earlier):
    tiles, rows, _ = q.shape
    half = near.shape[0]
    rr = near.shape[2]
    roots = 2 * half * CORES * rr
    qw = GROUPS * DH
    qrows = GROUPS * CHUNK
    first = earlier is None

    def low(t):
        return jnp.minimum(t, tiles - 1)

    def high(t):
        return jnp.maximum(t - tiles, 0)

    def col(info):
        return info[0] * HEADS + head

    whole = pl.BlockSpec(near.shape, lambda t, info: (0, 0, 0, 0))
    q_near_spec = pl.BlockSpec((1, rows, qw), lambda t, info: (low(t), 0, col(info)))
    q_far_spec = pl.BlockSpec((1, rows, qw), lambda t, info: (high(t), 0, head))
    db_near_spec = pl.BlockSpec((1, rows, b.shape[2]), lambda t, info: (low(t), 0, 0))
    db_far_spec = pl.BlockSpec((1, rows, b.shape[2]), lambda t, info: (high(t), 0, 0))
    in_specs = [
        q_near_spec,
        q_far_spec,
        q_near_spec,
        q_far_spec,
        pl.BlockSpec((1, rows, DH), lambda t, info: (low(t), 0, col(info))),
        pl.BlockSpec((1, rows, DH), lambda t, info: (high(t), 0, head)),
        pl.BlockSpec((1, rows, DH), lambda t, info: (low(t), 0, KVH + col(info))),
        pl.BlockSpec((1, rows, DH), lambda t, info: (high(t), 0, HEADS + head)),
        whole,
        whole,
    ]
    args = [q, q_far, g, g_far, b, b_far, b, b_far, near, nxt]
    aliases = {}
    if not first:
        any_spec = pl.BlockSpec(memory_space=pl.ANY)
        in_specs += [any_spec, any_spec, db_near_spec, db_far_spec]
        aliases = {1 + len(args) + i: i for i in range(4)}
        args += earlier
    out_specs = [q_near_spec, q_far_spec, db_near_spec, db_far_spec, whole, whole]
    out_shape = [
        jax.ShapeDtypeStruct(q.shape, BF16),
        jax.ShapeDtypeStruct((tiles, rows, HEADS * qw), BF16),
        jax.ShapeDtypeStruct(b.shape, BF16),
        jax.ShapeDtypeStruct(b.shape, BF16),
        jax.ShapeDtypeStruct(near.shape, F32),
        jax.ShapeDtypeStruct(near.shape, BF16),
    ]
    span = roots + rows
    scratch = [
        pltpu.VMEM((roots, DH), BF16),
        pltpu.VMEM((roots, DH), BF16),
        pltpu.VMEM((DH, roots), BF16),
        pltpu.VMEM((rows, DH), BF16),
        pltpu.VMEM((rows, DH), BF16),
        pltpu.VMEM((DH, rows), BF16),
        pltpu.VMEM((span, qrows), F32),
        pltpu.VMEM((span, qrows), F32),
        pltpu.VMEM((roots, DH), F32),
        pltpu.VMEM((roots, DH), F32),
        pltpu.VMEM((rows, DH), F32),
        pltpu.VMEM((rows, DH), F32),
        pltpu.VMEM((rows, qw), BF16),
    ]
    flops = 2 * 5 * tiles * rows * GROUPS * span * DH
    outs = pl.pallas_call(
        functools.partial(head_kernel, head, offsets, tiles),
        grid_spec=pltpu.PrefetchScalarGridSpec(
            num_scalar_prefetch=1,
            grid=(2 * tiles,),
            in_specs=in_specs,
            out_specs=out_specs,
            scratch_shapes=scratch,
        ),
        out_shape=out_shape,
        input_output_aliases=aliases,
        cost_estimate=pl.CostEstimate(
            flops=flops, bytes_accessed=8 * tiles * rows * qw, transcendentals=0
        ),
        compiler_params=pltpu.CompilerParams(dimension_semantics=("arbitrary",)),
    )(info, *args)
    return list(outs[:4]), outs[4], outs[5]


def local(query, grad_out, branch_kv, root_kv, lengths, segments):
    n_dev = lax.axis_size("dev")
    n_grp = lax.axis_size("grp")
    me = lax.axis_index("dev")
    core = me % CORES
    tiles, _, qcols = query.shape
    kcols = root_kv.shape[1] // 2
    offsets = tuple(range(0, n_dev, 2 * CORES))

    def cols(x, which, parts):
        part = x.shape[-1] // parts
        wide = part // CORES
        axis = x.ndim - 1
        pieces = [
            lax.dynamic_slice_in_dim(x, p * part + which * wide, wide, axis) for p in range(parts)
        ]
        return pieces

    mine = cols(root_kv, core, 2)
    other = jnp.concatenate(cols(root_kv, 1 - core, 2), axis=1)
    got = swapped(other, "dev", 1)
    got = [got[:, : kcols // CORES], got[:, kcols // CORES :]]
    gathered = []
    for head in range(HEADS):
        at = slice(head * DH, (head + 1) * DH)
        x = jnp.stack(
            [
                jnp.concatenate([mine[0][:, at], mine[1][:, at]], axis=1),
                jnp.concatenate([got[0][:, at], got[1][:, at]], axis=1),
            ]
        )[None]
        arrived = [swapped(x, "dev", off) for off in offsets[1:]]
        x = jnp.concatenate([x] + arrived, axis=0)
        nxt = swapped(x, "dev", CORES)
        gathered.append((x, nxt))

    q_far = swapped(cols(query, 1 - core, 1)[0], "dev", 1)
    g_far = swapped(cols(grad_out, 1 - core, 1)[0], "dev", 1)
    b_far = swapped(jnp.concatenate(cols(branch_kv, 1 - core, 2), axis=2), "dev", 1)
    meta = jnp.concatenate([lengths, segments]).reshape(2, tiles)
    meta_far = swapped(meta, "dev", 1)
    info = jnp.concatenate(
        [jnp.stack([core, me]), jnp.concatenate([meta, meta_far], axis=1).reshape(-1)]
    )

    outs = None
    sums = []
    for head in range(HEADS):
        near, nxt = gathered[head]
        outs, keep, send = head_grads(
            head, offsets, info, query, q_far, grad_out, g_far, branch_kv, b_far, near, nxt, outs
        )
        back = swapped(send, "dev", CORES)
        x = keep + back
        arrived = [swapped(x[j].astype(BF16), "dev", offsets[j]) for j in range(1, len(offsets))]
        x = x[0]
        for part in arrived:
            x = x + part
        sums.append(x)
    x = jnp.concatenate(sums, axis=2)
    hop = 1
    while hop < n_grp:
        x = x.astype(BF16)
        back = swapped(x, "grp", hop)
        x = x.astype(F32) + back.astype(F32)
        hop *= 2
    far = swapped(x[1], "dev", 1)
    near = x[0]
    pieces = []
    for part in range(2):
        for side in range(CORES):
            for head in range(HEADS):
                at = (head * 2 + part) * DH
                pieces.append(
                    jnp.where(core == side, near[:, at : at + DH], far[:, at : at + DH])
                )
    root_grad = jnp.concatenate(pieces, axis=1)

    dq, dq_far, db, db_far = outs
    dq_got = swapped(dq_far, "dev", 1)
    db_got = swapped(db_far, "dev", 1)
    query_grad = lax.dynamic_update_slice_in_dim(dq, dq_got, (1 - core) * (qcols // CORES), 2)
    col = lax.broadcasted_iota(jnp.int32, db.shape, 2)
    branch_grad = jnp.where(col // (HEADS * DH) % CORES == core, db, db_got)
    return (query_grad, branch_grad, root_grad)


def solution(mesh):
    placed = (
        P(("grp", "dev"), None, None),
        P(("grp", "dev"), None, None),
        P(("grp", "dev"), None, None),
        P("dev", None),
        P(("grp", "dev")),
        P(("grp", "dev")),
    )

    return jax.shard_map(
        local,
        mesh=mesh,
        in_specs=placed,
        out_specs=(P(("grp", "dev"), None, None), P(("grp", "dev"), None, None), P("dev", None)),
        check_vma=False,
    )
```

```python
import functools
import math

import jax
import jax.numpy as jnp
from jax import lax
from jax.experimental import pallas as pl
from jax.experimental.pallas import tpu as pltpu
from jax.sharding import PartitionSpec as P


H = 32
KVH = 4
DH = 128
SEGS = 4
GROUPS = H // KVH
CORES = 2
HEADS = KVH // CORES
CHUNK = 32
NT = (((1,), (1,)), ((), ()))
NN = (((1,), (0,)), ((), ()))
F32 = jnp.float32
BF16 = jnp.bfloat16


def swapped(block, axis, bit):
    route = [(i ^ bit, i) for i in range(lax.axis_size(axis))]
    return lax.ppermute(block, axis, route)


def dot(a, b, dims):
    return lax.dot_general(a, b, dims, preferred_element_type=F32)


def head_kernel(head, offsets, info, *refs):
    ins, refs = refs[:8], refs[-24:]
    q_own, q_far, g_own, g_far, b_own, b_far, kv_near, kv_next = ins
    dq_own, dq_far, db_own, db_far, keep, send = refs[:6]
    keys, values, keys_t, bkeys, bvalues, bkeys_t, s_scr, dp_scr = refs[6:14]
    dk_acc, dv_acc, dbk_acc, dbv_acc, q_buf, g_buf, dq_buf, db_buf = refs[14:22]
    in_sem, kv_sem = refs[22:]
    tiles, rows, _ = q_own.shape
    me = info[1]
    rr = kv_near.shape[2]
    roots = keys.shape[0]
    width = roots // SEGS
    qw = GROUPS * DH
    scale = DH ** (-0.5)
    sharp = scale * math.log2(math.e)
    at_own = pl.multiple_of((info[0] * HEADS + head) * qw, qw)
    k_own = pl.multiple_of((info[0] * HEADS + head) * DH, DH)

    def places():
        n = 0
        for side in range(2):
            for j, off in enumerate(offsets):
                for b0 in range(CORES):
                    rel = b0 + side * CORES + off
                    yield n, side, j, b0, pl.multiple_of((me ^ rel) * rr, rr)
                    n += 1

    def kv_copies():
        for n, side, j, b0, at in places():
            block = (kv_near, kv_next)[side].at[j, b0]
            for i, ref in enumerate((keys, values)):
                yield pltpu.make_async_copy(
                    block.at[:, pl.ds(i * DH, DH)], ref.at[pl.ds(at, rr)], kv_sem.at[n, i]
                )

    def tile_copies(t, out):
        if t < tiles:
            wide, narrow, at = pl.ds(at_own, qw), pl.ds(k_own, DH), t
            q_ref, g_ref, b_ref, dq_ref, db_ref = q_own, g_own, b_own, dq_own, db_own
            v_at = k_own + KVH * DH
        else:
            wide, narrow, at = pl.ds(head * qw, qw), pl.ds(head * DH, DH), t - tiles
            q_ref, g_ref, b_ref, dq_ref, db_ref = q_far, g_far, b_far, dq_far, db_far
            v_at = (HEADS + head) * DH
        v_narrow = pl.ds(v_at, DH)
        reads = (
            (q_ref.at[at, :, wide], q_buf.at[t]),
            (g_ref.at[at, :, wide], g_buf.at[t]),
            (b_ref.at[at, :, narrow], bkeys.at[t]),
            (b_ref.at[at, :, v_narrow], bvalues.at[t]),
        )
        writes = (
            (dq_buf.at[t], dq_ref.at[at, :, wide]),
            (db_buf.at[t, 0], db_ref.at[at, :, narrow]),
            (db_buf.at[t, 1], db_ref.at[at, :, v_narrow]),
        )
        picked = writes if out else reads
        return [
            pltpu.make_async_copy(src, dst, in_sem.at[t, i + (len(reads) if out else 0)])
            for i, (src, dst) in enumerate(picked)
        ]

    for copy in kv_copies():
        copy.start()
    for t in range(2 * tiles):

        @pl.when(info[2 + t] > 0)
        def _():
            for copy in tile_copies(t, False):
                copy.start()

    dk_acc[...] = jnp.zeros_like(dk_acc)
    dv_acc[...] = jnp.zeros_like(dv_acc)
    for copy in kv_copies():
        copy.wait()
    for b in range(0, roots, DH):
        keys_t[:, b : b + DH] = keys[b : b + DH, :].T

    def fold(x, op):
        return op(x.reshape(x.shape[0] // 8, 8, x.shape[1]), axis=0)

    def tile(t, carry):
        length = info[2 + t]
        segment = info[2 + 2 * tiles + t]

        dbk_acc[...] = jnp.zeros_like(dbk_acc)
        dbv_acc[...] = jnp.zeros_like(dbv_acc)

        for at in range(2 * tiles):

            @pl.when((t == at) & (length > 0))
            def _():
                for copy in tile_copies(at, False):
                    copy.wait()

        bkeys_t[...] = bkeys[t].T

        def piece(r0, size, segs):
            qrows = GROUPS * size
            lanes = slice(0, qrows)

            def stacked(ref):
                x = ref[t, pl.ds(r0, size), :]
                return jnp.concatenate([x[:, j * DH : (j + 1) * DH] for j in range(GROUPS)], axis=0)

            q = stacked(q_buf)
            g = stacked(g_buf)
            row = lax.broadcasted_iota(jnp.int32, (qrows, DH), 0) % size + r0
            g = jnp.where(row < length, g.astype(F32), 0.0).astype(BF16)

            spans = [(b * width, width) for b in range(segs)] + [(roots, rows)]
            ats = [slice(lo, lo + n) for lo, n in spans]

            def k_of(b):
                return keys[ats[b], :] if b < segs else bkeys[t]

            def v_of(b):
                return values[ats[b], :] if b < segs else bvalues[t]

            def kt_of(b):
                return keys_t[:, ats[b]] if b < segs else bkeys_t[...]

            top = None
            for b in range(segs + 1):
                s = dot(k_of(b), q, NT)
                if b == segs:
                    key = lax.broadcasted_iota(jnp.int32, s.shape, 0)
                    pos = lax.broadcasted_iota(jnp.int32, s.shape, 1) % size + r0
                    s = jnp.where(key <= pos, s, F32(-1e30))
                s_scr[ats[b], lanes] = s
                part = fold(s, jnp.max)
                top = part if top is None else jnp.maximum(top, part)
            peak = jnp.max(top, axis=0, keepdims=True)

            total = jnp.zeros((8, qrows), F32)
            for b in range(segs + 1):
                dp_scr[ats[b], lanes] = dot(v_of(b), g, NT)
                e = jnp.exp2((s_scr[ats[b], lanes] - peak) * sharp)
                s_scr[ats[b], lanes] = e
                total = total + fold(e, jnp.sum)
            inv = 1.0 / jnp.sum(total, axis=0, keepdims=True)

            delta = jnp.zeros((8, qrows), F32)
            for b in range(segs + 1):
                probs = (s_scr[ats[b], lanes] * inv).astype(BF16)
                delta = delta + fold(probs.astype(F32) * dp_scr[ats[b], lanes], jnp.sum)
                dv = dot(probs, g, NN)
                if b < segs:
                    dv_acc[ats[b], :] += dv
                else:
                    dbv_acc[...] += dv
            delta = jnp.sum(delta, axis=0, keepdims=True)
            invs = inv * scale

            dq_t = jnp.zeros((DH, qrows), F32)
            for b in range(segs + 1):
                ds = ((s_scr[ats[b], lanes] * invs) * (dp_scr[ats[b], lanes] - delta)).astype(BF16)
                dk = dot(ds, q, NN)
                if b < segs:
                    dk_acc[ats[b], :] += dk
                else:
                    dbk_acc[...] += dk
                dq_t = dq_t + dot(kt_of(b), ds, NN)
            dq = dq_t.T.astype(BF16)
            for j in range(GROUPS):
                dq_buf[t, pl.ds(r0, size), j * DH : (j + 1) * DH] = dq[j * size : (j + 1) * size, :]

        count = (length + (CHUNK - 1)) // CHUNK
        for s in range(SEGS):

            @pl.when(segment == s)
            def _():
                def step(c, carry):
                    piece(pl.multiple_of(c * (2 * CHUNK), 2 * CHUNK), 2 * CHUNK, s + 1)
                    return carry

                lax.fori_loop(0, count // 2, step, 0)

                @pl.when(count % 2 == 1)
                def _():
                    piece(pl.multiple_of((count - 1) * CHUNK, CHUNK), CHUNK, s + 1)

        def clear(c, carry):
            at = pl.multiple_of(c * CHUNK, CHUNK)
            dq_buf[t, pl.ds(at, CHUNK), :] = jnp.zeros((CHUNK, qw), BF16)
            return carry

        lax.fori_loop(count, rows // CHUNK, clear, 0)
        db_buf[t, 0] = dbk_acc[...].astype(BF16)
        db_buf[t, 1] = dbv_acc[...].astype(BF16)
        for at in range(2 * tiles):

            @pl.when(t == at)
            def _():
                for copy in tile_copies(at, True):
                    copy.start()

        return carry

    lax.fori_loop(0, 2 * tiles, tile, 0)

    for _, side, j, b0, at in places():
        out = (keep, send)[side]
        out[j, b0, :, :DH] = dk_acc[pl.ds(at, rr), :].astype(out.dtype)
        out[j, b0, :, DH:] = dv_acc[pl.ds(at, rr), :].astype(out.dtype)
    for t in range(2 * tiles):
        for copy in tile_copies(t, True):
            copy.wait()


def head_grads(head, offsets, info, q, q_far, g, g_far, b, b_far, near, nxt, earlier):
    tiles, rows, _ = q.shape
    half = near.shape[0]
    rr = near.shape[2]
    roots = 2 * half * CORES * rr
    qw = GROUPS * DH
    span = roots + rows
    vmem = pl.BlockSpec(memory_space=pltpu.VMEM)
    hbm = pl.BlockSpec(memory_space=pltpu.HBM)
    args = [q, q_far, g, g_far, b, b_far, near, nxt]
    in_specs = [pl.BlockSpec(memory_space=pltpu.SMEM)] + [hbm] * len(args)
    aliases = {}
    if earlier is not None:
        in_specs += [hbm] * 4
        aliases = {1 + len(args) + i: i for i in range(4)}
        args += earlier
    out_shape = [
        jax.ShapeDtypeStruct(q.shape, BF16),
        jax.ShapeDtypeStruct((tiles, rows, HEADS * qw), BF16),
        jax.ShapeDtypeStruct(b.shape, BF16),
        jax.ShapeDtypeStruct(b_far.shape, BF16),
        jax.ShapeDtypeStruct(near.shape, F32),
        jax.ShapeDtypeStruct(near.shape, BF16),
    ]
    scratch = [
        pltpu.VMEM((roots, DH), BF16),
        pltpu.VMEM((roots, DH), BF16),
        pltpu.VMEM((DH, roots), BF16),
        pltpu.VMEM((2 * tiles, rows, DH), BF16),
        pltpu.VMEM((2 * tiles, rows, DH), BF16),
        pltpu.VMEM((DH, rows), BF16),
        pltpu.VMEM((span, 2 * CHUNK * GROUPS), F32),
        pltpu.VMEM((span, 2 * CHUNK * GROUPS), F32),
        pltpu.VMEM((roots, DH), F32),
        pltpu.VMEM((roots, DH), F32),
        pltpu.VMEM((rows, DH), F32),
        pltpu.VMEM((rows, DH), F32),
        pltpu.VMEM((2 * tiles, rows, qw), BF16),
        pltpu.VMEM((2 * tiles, rows, qw), BF16),
        pltpu.VMEM((2 * tiles, rows, qw), BF16),
        pltpu.VMEM((2 * tiles, 2, rows, DH), BF16),
        pltpu.SemaphoreType.DMA((2 * tiles, 7)),
        pltpu.SemaphoreType.DMA((2 * half * CORES, 2)),
    ]
    flops = 2 * 5 * tiles * rows * GROUPS * span * DH
    outs = pl.pallas_call(
        functools.partial(head_kernel, head, offsets),
        in_specs=in_specs,
        out_specs=[hbm] * 4 + [vmem] * 2,
        scratch_shapes=scratch,
        out_shape=out_shape,
        input_output_aliases=aliases,
        cost_estimate=pl.CostEstimate(
            flops=flops, bytes_accessed=8 * tiles * rows * qw, transcendentals=0
        ),
        compiler_params=pltpu.CompilerParams(vmem_limit_bytes=32 * 2**20),
    )(info, *args)
    return list(outs[:4]), outs[4], outs[5]


def local(query, grad_out, branch_kv, root_kv, lengths, segments):
    n_dev = lax.axis_size("dev")
    n_grp = lax.axis_size("grp")
    me = lax.axis_index("dev")
    core = me % CORES
    tiles, _, qcols = query.shape
    kcols = root_kv.shape[1] // 2
    offsets = tuple(range(0, n_dev, 2 * CORES))

    def cols(x, which, parts):
        part = x.shape[-1] // parts
        wide = part // CORES
        axis = x.ndim - 1
        pieces = [
            lax.dynamic_slice_in_dim(x, p * part + which * wide, wide, axis) for p in range(parts)
        ]
        return pieces

    mine = cols(root_kv, core, 2)
    other = jnp.concatenate(cols(root_kv, 1 - core, 2), axis=1)
    got = swapped(other, "dev", 1)
    got = [got[:, : kcols // CORES], got[:, kcols // CORES :]]
    gathered = []
    for head in range(HEADS):
        at = slice(head * DH, (head + 1) * DH)
        x = jnp.stack(
            [
                jnp.concatenate([mine[0][:, at], mine[1][:, at]], axis=1),
                jnp.concatenate([got[0][:, at], got[1][:, at]], axis=1),
            ]
        )[None]
        arrived = [swapped(x, "dev", off) for off in offsets[1:]]
        x = jnp.concatenate([x] + arrived, axis=0)
        nxt = swapped(x, "dev", CORES)
        gathered.append((x, nxt))

    q_far = swapped(cols(query, 1 - core, 1)[0], "dev", 1)
    g_far = swapped(cols(grad_out, 1 - core, 1)[0], "dev", 1)
    b_far = swapped(jnp.concatenate(cols(branch_kv, 1 - core, 2), axis=2), "dev", 1)
    meta = jnp.concatenate([lengths, segments]).reshape(2, tiles)
    meta_far = swapped(meta, "dev", 1)
    info = jnp.concatenate(
        [jnp.stack([core, me]), jnp.concatenate([meta, meta_far], axis=1).reshape(-1)]
    )

    outs = None
    sums = []
    for head in range(HEADS):
        near, nxt = gathered[head]
        outs, keep, send = head_grads(
            head, offsets, info, query, q_far, grad_out, g_far, branch_kv, b_far, near, nxt, outs
        )
        back = swapped(send, "dev", CORES)
        x = keep + back
        arrived = [swapped(x[j].astype(BF16), "dev", offsets[j]) for j in range(1, len(offsets))]
        x = x[0]
        for part in arrived:
            x = x + part
        sums.append(x)
    x = jnp.concatenate(sums, axis=2)
    hop = 1
    while hop < n_grp:
        x = x.astype(BF16)
        back = swapped(x, "grp", hop)
        x = x.astype(F32) + back.astype(F32)
        hop *= 2
    far = swapped(x[1], "dev", 1)
    near = x[0]
    pieces = []
    for part in range(2):
        for side in range(CORES):
            for head in range(HEADS):
                at = (head * 2 + part) * DH
                pieces.append(
                    jnp.where(core == side, near[:, at : at + DH], far[:, at : at + DH])
                )
    root_grad = jnp.concatenate(pieces, axis=1)

    dq, dq_far, db, db_far = outs
    dq_got = swapped(dq_far, "dev", 1)
    db_got = swapped(db_far, "dev", 1)
    query_grad = lax.dynamic_update_slice_in_dim(dq, dq_got, (1 - core) * (qcols // CORES), 2)
    wide = HEADS * DH
    branch_grad = db
    for part in range(2):
        branch_grad = lax.dynamic_update_slice_in_dim(
            branch_grad,
            db_got[:, :, part * wide : (part + 1) * wide],
            (part * CORES + 1 - core) * wide,
            2,
        )
    return (query_grad, branch_grad, root_grad)


def solution(mesh):
    placed = (
        P(("grp", "dev"), None, None),
        P(("grp", "dev"), None, None),
        P(("grp", "dev"), None, None),
        P("dev", None),
        P(("grp", "dev")),
        P(("grp", "dev")),
    )

    return jax.shard_map(
        local,
        mesh=mesh,
        in_specs=placed,
        out_specs=(P(("grp", "dev"), None, None), P(("grp", "dev"), None, None), P("dev", None)),
        check_vma=False,
    )
```

```python
import functools
import math

import jax
import jax.numpy as jnp
from jax import lax
from jax.experimental import pallas as pl
from jax.experimental.pallas import tpu as pltpu
from jax.sharding import PartitionSpec as P


H = 32
KVH = 4
DH = 128
SEGS = 4
GROUPS = H // KVH
CORES = 2
HEADS = KVH // CORES
CHUNK = 32
NT = (((1,), (1,)), ((), ()))
NN = (((1,), (0,)), ((), ()))
F32 = jnp.float32
BF16 = jnp.bfloat16


def swapped(block, axis, bit):
    route = [(i ^ bit, i) for i in range(lax.axis_size(axis))]
    return lax.ppermute(block, axis, route)


def dot(a, b, dims):
    return lax.dot_general(a, b, dims, preferred_element_type=F32)


def head_kernel(head, offsets, info, *refs):
    ins, refs = refs[:8], refs[-24:]
    q_own, q_far, g_own, g_far, b_own, b_far, kv_near, kv_next = ins
    dq_own, dq_far, db_own, db_far, keep, send = refs[:6]
    keys, values, keys_t, bkeys, bvalues, bkeys_t, s_scr, dp_scr = refs[6:14]
    dk_acc, dv_acc, dbk_acc, dbv_acc, q_buf, g_buf, dq_buf, db_buf = refs[14:22]
    in_sem, kv_sem = refs[22:]
    tiles, rows, _ = q_own.shape
    me = info[1]
    rr = kv_near.shape[2]
    roots = keys.shape[0]
    width = roots // SEGS
    qw = GROUPS * DH
    scale = DH ** (-0.5)
    sharp = scale * math.log2(math.e)
    at_own = pl.multiple_of((info[0] * HEADS + head) * qw, qw)
    k_own = pl.multiple_of((info[0] * HEADS + head) * DH, DH)

    def places():
        n = 0
        for side in range(2):
            for j, off in enumerate(offsets):
                for b0 in range(CORES):
                    rel = b0 + side * CORES + off
                    yield n, side, j, b0, pl.multiple_of((me ^ rel) * rr, rr)
                    n += 1

    def kv_copies():
        for n, side, j, b0, at in places():
            block = (kv_near, kv_next)[side].at[j, b0]
            for i, ref in enumerate((keys, values)):
                yield pltpu.make_async_copy(
                    block.at[:, pl.ds(i * DH, DH)], ref.at[pl.ds(at, rr)], kv_sem.at[n, i]
                )

    def tile_copies(t, out):
        if t < tiles:
            wide, narrow, at = pl.ds(at_own, qw), pl.ds(k_own, DH), t
            q_ref, g_ref, b_ref, dq_ref, db_ref = q_own, g_own, b_own, dq_own, db_own
            v_at = k_own + KVH * DH
        else:
            wide, narrow, at = pl.ds(head * qw, qw), pl.ds(head * DH, DH), t - tiles
            q_ref, g_ref, b_ref, dq_ref, db_ref = q_far, g_far, b_far, dq_far, db_far
            v_at = (HEADS + head) * DH
        v_narrow = pl.ds(v_at, DH)
        reads = (
            (q_ref.at[at, :, wide], q_buf.at[t]),
            (g_ref.at[at, :, wide], g_buf.at[t]),
            (b_ref.at[at, :, narrow], bkeys.at[t]),
            (b_ref.at[at, :, v_narrow], bvalues.at[t]),
        )
        writes = (
            (dq_buf.at[t], dq_ref.at[at, :, wide]),
            (db_buf.at[t, 0], db_ref.at[at, :, narrow]),
            (db_buf.at[t, 1], db_ref.at[at, :, v_narrow]),
        )
        picked = writes if out else reads
        return [
            pltpu.make_async_copy(src, dst, in_sem.at[t, i + (len(reads) if out else 0)])
            for i, (src, dst) in enumerate(picked)
        ]

    for copy in kv_copies():
        copy.start()
    for t in range(2 * tiles):

        @pl.when(info[2 + t] > 0)
        def _():
            for copy in tile_copies(t, False):
                copy.start()

    dk_acc[...] = jnp.zeros_like(dk_acc)
    dv_acc[...] = jnp.zeros_like(dv_acc)
    for copy in kv_copies():
        copy.wait()
    for b in range(0, roots, DH):
        keys_t[:, b : b + DH] = keys[b : b + DH, :].T

    def fold(x, op):
        return op(x.reshape(x.shape[0] // 8, 8, x.shape[1]), axis=0)

    def tile(t, carry):
        length = info[2 + t]
        segment = info[2 + 2 * tiles + t]

        dbk_acc[...] = jnp.zeros_like(dbk_acc)
        dbv_acc[...] = jnp.zeros_like(dbv_acc)

        for at in range(2 * tiles):

            @pl.when((t == at) & (length > 0))
            def _():
                for copy in tile_copies(at, False):
                    copy.wait()

        bkeys_t[...] = bkeys[t].T

        def piece(r0, size, segs):
            qrows = GROUPS * size
            lanes = slice(0, qrows)

            def stacked(ref):
                x = ref[t, pl.ds(r0, size), :]
                return jnp.concatenate([x[:, j * DH : (j + 1) * DH] for j in range(GROUPS)], axis=0)

            q = stacked(q_buf)
            g = stacked(g_buf)
            row = lax.broadcasted_iota(jnp.int32, (qrows, DH), 0) % size + r0
            g = jnp.where(row < length, g.astype(F32), 0.0).astype(BF16)

            spans = [(b * width, width) for b in range(segs)] + [(roots, rows)]
            ats = [slice(lo, lo + n) for lo, n in spans]

            def k_of(b):
                return keys[ats[b], :] if b < segs else bkeys[t]

            def v_of(b):
                return values[ats[b], :] if b < segs else bvalues[t]

            def kt_of(b):
                return keys_t[:, ats[b]] if b < segs else bkeys_t[...]

            top = None
            for b in range(segs + 1):
                s = dot(k_of(b), q, NT)
                if b == segs:
                    key = lax.broadcasted_iota(jnp.int32, s.shape, 0)
                    pos = lax.broadcasted_iota(jnp.int32, s.shape, 1) % size + r0
                    s = jnp.where(key <= pos, s, F32(-1e30))
                s_scr[ats[b], lanes] = s
                part = fold(s, jnp.max)
                top = part if top is None else jnp.maximum(top, part)
            peak = jnp.max(top, axis=0, keepdims=True)

            total = jnp.zeros((8, qrows), F32)
            for b in range(segs + 1):
                dp_scr[ats[b], lanes] = dot(v_of(b), g, NT)
                e = jnp.exp2((s_scr[ats[b], lanes] - peak) * sharp)
                s_scr[ats[b], lanes] = e
                total = total + fold(e, jnp.sum)
            inv = 1.0 / jnp.sum(total, axis=0, keepdims=True)

            delta = jnp.zeros((8, qrows), F32)
            for b in range(segs + 1):
                probs = (s_scr[ats[b], lanes] * inv).astype(BF16)
                delta = delta + fold(probs.astype(F32) * dp_scr[ats[b], lanes], jnp.sum)
                dv = dot(probs, g, NN)
                if b < segs:
                    dv_acc[ats[b], :] += dv
                else:
                    dbv_acc[...] += dv
            delta = jnp.sum(delta, axis=0, keepdims=True)
            invs = inv * scale

            dq_t = jnp.zeros((DH, qrows), F32)
            for b in range(segs + 1):
                ds = ((s_scr[ats[b], lanes] * invs) * (dp_scr[ats[b], lanes] - delta)).astype(BF16)
                dk = dot(ds, q, NN)
                if b < segs:
                    dk_acc[ats[b], :] += dk
                else:
                    dbk_acc[...] += dk
                dq_t = dq_t + dot(kt_of(b), ds, NN)
            dq = dq_t.T.astype(BF16)
            for j in range(GROUPS):
                dq_buf[t, pl.ds(r0, size), j * DH : (j + 1) * DH] = dq[j * size : (j + 1) * size, :]

        count = (length + (CHUNK - 1)) // CHUNK
        for s in range(SEGS):

            @pl.when(segment == s)
            def _():
                def step(c, carry):
                    piece(pl.multiple_of(c * (2 * CHUNK), 2 * CHUNK), 2 * CHUNK, s + 1)
                    return carry

                lax.fori_loop(0, count // 2, step, 0)

                @pl.when(count % 2 == 1)
                def _():
                    piece(pl.multiple_of((count - 1) * CHUNK, CHUNK), CHUNK, s + 1)

        def clear(c, carry):
            at = pl.multiple_of(c * CHUNK, CHUNK)
            dq_buf[t, pl.ds(at, CHUNK), :] = jnp.zeros((CHUNK, qw), BF16)
            return carry

        lax.fori_loop(count, rows // CHUNK, clear, 0)
        db_buf[t, 0] = dbk_acc[...].astype(BF16)
        db_buf[t, 1] = dbv_acc[...].astype(BF16)
        for at in range(2 * tiles):

            @pl.when(t == at)
            def _():
                for copy in tile_copies(at, True):
                    copy.start()

        return carry

    lax.fori_loop(0, 2 * tiles, tile, 0)

    for _, side, j, b0, at in places():
        out = (keep, send)[side]
        out[j, b0, :, :DH] = dk_acc[pl.ds(at, rr), :].astype(out.dtype)
        out[j, b0, :, DH:] = dv_acc[pl.ds(at, rr), :].astype(out.dtype)
    for t in range(2 * tiles):
        for copy in tile_copies(t, True):
            copy.wait()


def head_grads(head, offsets, info, q, q_far, g, g_far, b, b_far, near, nxt, earlier):
    tiles, rows, _ = q.shape
    half = near.shape[0]
    rr = near.shape[2]
    roots = 2 * half * CORES * rr
    qw = GROUPS * DH
    span = roots + rows
    vmem = pl.BlockSpec(memory_space=pltpu.VMEM)
    hbm = pl.BlockSpec(memory_space=pltpu.HBM)
    q, g, b = (pltpu.with_memory_space_constraint(x, pltpu.HBM) for x in (q, g, b))
    args = [q, q_far, g, g_far, b, b_far, near, nxt]
    in_specs = [pl.BlockSpec(memory_space=pltpu.SMEM)] + [hbm] * len(args)
    aliases = {}
    if earlier is not None:
        in_specs += [hbm] * 4
        aliases = {1 + len(args) + i: i for i in range(4)}
        args += earlier
    out_shape = [
        jax.ShapeDtypeStruct(q.shape, BF16),
        jax.ShapeDtypeStruct((tiles, rows, HEADS * qw), BF16),
        jax.ShapeDtypeStruct(b.shape, BF16),
        jax.ShapeDtypeStruct(b_far.shape, BF16),
        jax.ShapeDtypeStruct(near.shape, F32),
        jax.ShapeDtypeStruct(near.shape, BF16),
    ]
    scratch = [
        pltpu.VMEM((roots, DH), BF16),
        pltpu.VMEM((roots, DH), BF16),
        pltpu.VMEM((DH, roots), BF16),
        pltpu.VMEM((2 * tiles, rows, DH), BF16),
        pltpu.VMEM((2 * tiles, rows, DH), BF16),
        pltpu.VMEM((DH, rows), BF16),
        pltpu.VMEM((span, 2 * CHUNK * GROUPS), F32),
        pltpu.VMEM((span, 2 * CHUNK * GROUPS), F32),
        pltpu.VMEM((roots, DH), F32),
        pltpu.VMEM((roots, DH), F32),
        pltpu.VMEM((rows, DH), F32),
        pltpu.VMEM((rows, DH), F32),
        pltpu.VMEM((2 * tiles, rows, qw), BF16),
        pltpu.VMEM((2 * tiles, rows, qw), BF16),
        pltpu.VMEM((2 * tiles, rows, qw), BF16),
        pltpu.VMEM((2 * tiles, 2, rows, DH), BF16),
        pltpu.SemaphoreType.DMA((2 * tiles, 7)),
        pltpu.SemaphoreType.DMA((2 * half * CORES, 2)),
    ]
    flops = 2 * 5 * tiles * rows * GROUPS * span * DH
    outs = pl.pallas_call(
        functools.partial(head_kernel, head, offsets),
        in_specs=in_specs,
        out_specs=[hbm] * 4 + [vmem] * 2,
        scratch_shapes=scratch,
        out_shape=out_shape,
        input_output_aliases=aliases,
        cost_estimate=pl.CostEstimate(
            flops=flops, bytes_accessed=8 * tiles * rows * qw, transcendentals=0
        ),
        compiler_params=pltpu.CompilerParams(vmem_limit_bytes=32 * 2**20),
    )(info, *args)
    return list(outs[:4]), outs[4], outs[5]


def local(query, grad_out, branch_kv, root_kv, lengths, segments):
    n_dev = lax.axis_size("dev")
    n_grp = lax.axis_size("grp")
    me = lax.axis_index("dev")
    core = me % CORES
    tiles, _, qcols = query.shape
    kcols = root_kv.shape[1] // 2
    offsets = tuple(range(0, n_dev, 2 * CORES))

    def cols(x, which, parts):
        part = x.shape[-1] // parts
        wide = part // CORES
        axis = x.ndim - 1
        pieces = [
            lax.dynamic_slice_in_dim(x, p * part + which * wide, wide, axis) for p in range(parts)
        ]
        return pieces

    mine = cols(root_kv, core, 2)
    other = jnp.concatenate(cols(root_kv, 1 - core, 2), axis=1)
    got = swapped(other, "dev", 1)
    got = [got[:, : kcols // CORES], got[:, kcols // CORES :]]
    gathered = []
    for head in range(HEADS):
        at = slice(head * DH, (head + 1) * DH)
        x = jnp.stack(
            [
                jnp.concatenate([mine[0][:, at], mine[1][:, at]], axis=1),
                jnp.concatenate([got[0][:, at], got[1][:, at]], axis=1),
            ]
        )[None]
        arrived = [swapped(x, "dev", off) for off in offsets[1:]]
        x = jnp.concatenate([x] + arrived, axis=0)
        nxt = swapped(x, "dev", CORES)
        gathered.append((x, nxt))

    q_far = swapped(cols(query, 1 - core, 1)[0], "dev", 1)
    g_far = swapped(cols(grad_out, 1 - core, 1)[0], "dev", 1)
    b_far = swapped(jnp.concatenate(cols(branch_kv, 1 - core, 2), axis=2), "dev", 1)
    meta = jnp.concatenate([lengths, segments]).reshape(2, tiles)
    meta_far = swapped(meta, "dev", 1)
    info = jnp.concatenate(
        [jnp.stack([core, me]), jnp.concatenate([meta, meta_far], axis=1).reshape(-1)]
    )

    outs = None
    sums = []
    for head in range(HEADS):
        near, nxt = gathered[head]
        outs, keep, send = head_grads(
            head, offsets, info, query, q_far, grad_out, g_far, branch_kv, b_far, near, nxt, outs
        )
        back = swapped(send, "dev", CORES)
        x = keep + back
        arrived = [swapped(x[j].astype(BF16), "dev", offsets[j]) for j in range(1, len(offsets))]
        x = x[0]
        for part in arrived:
            x = x + part
        sums.append(x)
    x = jnp.concatenate(
        [s[:, :, part * DH : (part + 1) * DH] for part in range(2) for s in sums], axis=2
    )
    hop = 1
    while hop < n_grp:
        x = x.astype(BF16)
        back = swapped(x, "grp", hop)
        x = x.astype(F32) + back.astype(F32)
        hop *= 2
    far = swapped(x[1], "dev", 1)
    near = x[0]
    wide = HEADS * DH
    pieces = []
    for part in range(2):
        at = slice(part * wide, (part + 1) * wide)
        for side in range(CORES):
            pieces.append(jnp.where(core == side, near[:, at], far[:, at]))
    root_grad = jnp.concatenate(pieces, axis=1)

    dq, dq_far, db, db_far = outs
    dq_got = swapped(dq_far, "dev", 1)
    db_got = swapped(db_far, "dev", 1)
    query_grad = lax.dynamic_update_slice_in_dim(dq, dq_got, (1 - core) * (qcols // CORES), 2)
    branch_grad = db
    for part in range(2):
        branch_grad = lax.dynamic_update_slice_in_dim(
            branch_grad,
            db_got[:, :, part * wide : (part + 1) * wide],
            (part * CORES + 1 - core) * wide,
            2,
        )
    return (query_grad, branch_grad, root_grad)


def solution(mesh):
    placed = (
        P(("grp", "dev"), None, None),
        P(("grp", "dev"), None, None),
        P(("grp", "dev"), None, None),
        P("dev", None),
        P(("grp", "dev")),
        P(("grp", "dev")),
    )

    return jax.shard_map(
        local,
        mesh=mesh,
        in_specs=placed,
        out_specs=(P(("grp", "dev"), None, None), P(("grp", "dev"), None, None), P("dev", None)),
        check_vma=False,
    )
```

```python
import functools
import math

import jax
import jax.numpy as jnp
from jax import lax
from jax.experimental import pallas as pl
from jax.experimental.pallas import tpu as pltpu
from jax.sharding import PartitionSpec as P


H = 32
KVH = 4
DH = 128
SEGS = 4
GROUPS = H // KVH
CORES = 2
HEADS = KVH // CORES
CHUNK = 32
BLOCK = 256
NT = (((1,), (1,)), ((), ()))
NN = (((1,), (0,)), ((), ()))
F32 = jnp.float32
BF16 = jnp.bfloat16


def swapped(block, axis, bit):
    route = [(i ^ bit, i) for i in range(lax.axis_size(axis))]
    return lax.ppermute(block, axis, route)


def dot(a, b, dims):
    return lax.dot_general(a, b, dims, preferred_element_type=F32)


def head_kernel(head, offsets, len_own, len_far, seg_own, seg_far, *refs):
    ins, refs = refs[:8], refs[-22:]
    q_own, q_far, g_own, g_far, b_own, b_far, kv_near, kv_next = ins
    dq_own, dq_far, db_own, db_far, keep, send = refs[:6]
    pairs, keys_t, bkeys, bvalues, bkeys_t, s_scr, dp_scr = refs[6:13]
    dk_acc, dv_acc, dbk_acc, dbv_acc, q_buf, g_buf, dq_buf, db_buf = refs[13:21]
    in_sem = refs[21]
    tiles, rows, _ = q_own.shape
    me = lax.axis_index("dev")
    core = me % CORES
    rr = kv_near.shape[2]
    roots = pairs.shape[0]
    width = roots // SEGS
    qw = GROUPS * DH
    scale = DH ** (-0.5)
    sharp = scale * math.log2(math.e)
    wide = pl.ds(pl.multiple_of((core * HEADS + head) * qw, qw), qw)
    narrow = pl.ds(pl.multiple_of((core * HEADS + head) * DH, DH), DH)
    v_narrow = pl.ds(pl.multiple_of((KVH + core * HEADS + head) * DH, DH), DH)

    def picked(t, near_ref, far_ref):
        near = near_ref[jnp.minimum(t, tiles - 1)]
        return jnp.where(t < tiles, near, far_ref[jnp.maximum(t - tiles, 0)])

    def places():
        n = 0
        for side in range(2):
            for j, off in enumerate(offsets):
                for b0 in range(CORES):
                    rel = b0 + side * CORES + off
                    yield n, side, j, b0, pl.multiple_of((me ^ rel) * rr, rr)
                    n += 1

    def tile_copies(t, out):
        if t < tiles:
            q_ref, g_ref, b_ref, dq_ref, db_ref = q_own, g_own, b_own, dq_own, db_own
            at, dq_at, db_at, dv_at = t, wide, narrow, v_narrow
        else:
            q_ref, g_ref, b_ref, dq_ref, db_ref = q_far, g_far, b_far, dq_far, db_far
            at, dq_at = t - tiles, pl.ds(head * qw, qw)
            db_at, dv_at = pl.ds(head * DH, DH), pl.ds((HEADS + head) * DH, DH)
        reads = (
            (q_ref.at[at, :, wide], q_buf.at[t]),
            (g_ref.at[at, :, wide], g_buf.at[t]),
            (b_ref.at[at, :, narrow], bkeys.at[t]),
            (b_ref.at[at, :, v_narrow], bvalues.at[t]),
        )
        writes = (
            (dq_buf.at[t], dq_ref.at[at, :, dq_at]),
            (db_buf.at[t, 0], db_ref.at[at, :, db_at]),
            (db_buf.at[t, 1], db_ref.at[at, :, dv_at]),
        )
        chosen = writes if out else reads
        return [
            pltpu.make_async_copy(src, dst, in_sem.at[t, i + (len(reads) if out else 0)])
            for i, (src, dst) in enumerate(chosen)
        ]

    for t in range(2 * tiles):

        @pl.when(picked(t, len_own, len_far) > 0)
        def _():
            for copy in tile_copies(t, False):
                copy.start()

    dk_acc[...] = jnp.zeros_like(dk_acc)
    dv_acc[...] = jnp.zeros_like(dv_acc)
    for _, side, j, b0, at in places():
        pairs[pl.ds(at, rr), :] = (kv_near, kv_next)[side][j, b0]
    for b in range(0, roots, DH):
        keys_t[:, b : b + DH] = pairs[b : b + DH, :DH].T

    def fold(x, op):
        return op(x.reshape(x.shape[0] // 8, 8, x.shape[1]), axis=0)

    def tile(t, carry):
        length = picked(t, len_own, len_far)
        segment = picked(t, seg_own, seg_far)

        dbk_acc[...] = jnp.zeros_like(dbk_acc)
        dbv_acc[...] = jnp.zeros_like(dbv_acc)

        for at in range(2 * tiles):

            @pl.when((t == at) & (length > 0))
            def _():
                for copy in tile_copies(at, False):
                    copy.wait()

        bkeys_t[...] = bkeys[t].T

        def pieces(starts, segs):
            size = CHUNK
            qrows = GROUPS * size
            every = range(len(starts))
            lanes = [slice(i * qrows, (i + 1) * qrows) for i in every]
            count = segs * width // BLOCK
            spans = [(b * BLOCK, BLOCK) for b in range(count)] + [(roots, rows)]
            ats = [slice(lo, lo + n) for lo, n in spans]

            def stacked(ref, r0):
                x = ref[t, pl.ds(r0, size), :]
                return jnp.concatenate([x[:, j * DH : (j + 1) * DH] for j in range(GROUPS)], axis=0)

            def masked(g, r0):
                row = lax.broadcasted_iota(jnp.int32, (qrows, DH), 0) % size + r0
                return jnp.where(row < length, g.astype(F32), 0.0).astype(BF16)

            q = [stacked(q_buf, r0) for r0 in starts]
            g = [masked(stacked(g_buf, r0), r0) for r0 in starts]

            def k_of(b):
                return pairs[ats[b], :DH] if b < count else bkeys[t]

            def v_of(b):
                return pairs[ats[b], DH:] if b < count else bvalues[t]

            def kt_of(b):
                return keys_t[:, ats[b]] if b < count else bkeys_t[...]

            peaks, invs = [], []
            for i in every:
                top = None
                for b in range(count + 1):
                    s = dot(k_of(b), q[i], NT)
                    if b == count:
                        key = lax.broadcasted_iota(jnp.int32, s.shape, 0)
                        pos = lax.broadcasted_iota(jnp.int32, s.shape, 1) % size + starts[i]
                        s = jnp.where(key <= pos, s, F32(-1e30))
                    s_scr[ats[b], lanes[i]] = s
                    part = fold(s, jnp.max)
                    top = part if top is None else jnp.maximum(top, part)
                peaks.append(jnp.max(top, axis=0, keepdims=True))

            for i in every:
                total = jnp.zeros((8, qrows), F32)
                for b in range(count + 1):
                    dp_scr[ats[b], lanes[i]] = dot(v_of(b), g[i], NT)
                    e = jnp.exp2((s_scr[ats[b], lanes[i]] - peaks[i]) * sharp)
                    s_scr[ats[b], lanes[i]] = e
                    total = total + fold(e, jnp.sum)
                invs.append(1.0 / jnp.sum(total, axis=0, keepdims=True))

            deltas = []
            for i in every:
                delta = jnp.zeros((8, qrows), F32)
                for b in range(count + 1):
                    probs = (s_scr[ats[b], lanes[i]] * invs[i]).astype(BF16)
                    delta = delta + fold(probs.astype(F32) * dp_scr[ats[b], lanes[i]], jnp.sum)
                    dv = dot(probs, g[i], NN)
                    if b < count:
                        dv_acc[ats[b], :] += dv
                    else:
                        dbv_acc[...] += dv
                deltas.append(jnp.sum(delta, axis=0, keepdims=True))

            for i in every:
                dq_t = jnp.zeros((DH, qrows), F32)
                scaled = invs[i] * scale
                for b in range(count + 1):
                    ds = (s_scr[ats[b], lanes[i]] * scaled) * (dp_scr[ats[b], lanes[i]] - deltas[i])
                    ds = ds.astype(BF16)
                    dk = dot(ds, q[i], NN)
                    if b < count:
                        dk_acc[ats[b], :] += dk
                    else:
                        dbk_acc[...] += dk
                    dq_t = dq_t + dot(kt_of(b), ds, NN)
                dq = dq_t.T.astype(BF16)
                for j in range(GROUPS):
                    part = dq[j * size : (j + 1) * size, :]
                    dq_buf[t, pl.ds(starts[i], size), j * DH : (j + 1) * DH] = part

        count = (length + (CHUNK - 1)) // CHUNK
        for s in range(SEGS):

            @pl.when(segment == s)
            def _():
                def step(c, carry):
                    first = c * (2 * CHUNK)
                    pieces([pl.multiple_of(first + i * CHUNK, CHUNK) for i in range(2)], s + 1)
                    return carry

                lax.fori_loop(0, count // 2, step, 0)

                @pl.when(count % 2 == 1)
                def _():
                    pieces([pl.multiple_of((count - 1) * CHUNK, CHUNK)], s + 1)

        def clear(c, carry):
            at = pl.multiple_of(c * CHUNK, CHUNK)
            dq_buf[t, pl.ds(at, CHUNK), :] = jnp.zeros((CHUNK, qw), BF16)
            return carry

        lax.fori_loop(count, rows // CHUNK, clear, 0)
        db_buf[t, 0] = dbk_acc[...].astype(BF16)
        db_buf[t, 1] = dbv_acc[...].astype(BF16)
        for at in range(2 * tiles):

            @pl.when(t == at)
            def _():
                for copy in tile_copies(at, True):
                    copy.start()

        return carry

    lax.fori_loop(0, 2 * tiles, tile, 0)

    for _, side, j, b0, at in places():
        out = (keep, send)[side]
        out[j, b0, :, :DH] = dk_acc[pl.ds(at, rr), :].astype(out.dtype)
        out[j, b0, :, DH:] = dv_acc[pl.ds(at, rr), :].astype(out.dtype)
    for t in range(2 * tiles):
        for copy in tile_copies(t, True):
            copy.wait()


def head_grads(head, offsets, meta, q, q_far, g, g_far, b, b_far, near, nxt, earlier):
    tiles, rows, _ = q.shape
    half = near.shape[0]
    rr = near.shape[2]
    roots = 2 * half * CORES * rr
    qw = GROUPS * DH
    span = roots + rows
    vmem = pl.BlockSpec(memory_space=pltpu.VMEM)
    hbm = pl.BlockSpec(memory_space=pltpu.HBM)
    q, g, b = (pltpu.with_memory_space_constraint(x, pltpu.HBM) for x in (q, g, b))
    args = [q, q_far, g, g_far, b, b_far, near, nxt]
    in_specs = [pl.BlockSpec(memory_space=pltpu.SMEM)] * len(meta) + [hbm] * 6 + [vmem] * 2
    aliases = {}
    if earlier is not None:
        in_specs += [hbm] * 4
        aliases = {len(meta) + len(args) + i: i for i in range(4)}
        args += earlier
    out_shape = [
        jax.ShapeDtypeStruct(q.shape, BF16),
        jax.ShapeDtypeStruct((tiles, rows, HEADS * qw), BF16),
        jax.ShapeDtypeStruct(b.shape, BF16),
        jax.ShapeDtypeStruct((tiles, rows, 2 * HEADS * DH), BF16),
        jax.ShapeDtypeStruct(near.shape, F32),
        jax.ShapeDtypeStruct(near.shape, BF16),
    ]
    scratch = [
        pltpu.VMEM((roots, 2 * DH), BF16),
        pltpu.VMEM((DH, roots), BF16),
        pltpu.VMEM((2 * tiles, rows, DH), BF16),
        pltpu.VMEM((2 * tiles, rows, DH), BF16),
        pltpu.VMEM((DH, rows), BF16),
        pltpu.VMEM((span, 2 * CHUNK * GROUPS), F32),
        pltpu.VMEM((span, 2 * CHUNK * GROUPS), F32),
        pltpu.VMEM((roots, DH), F32),
        pltpu.VMEM((roots, DH), F32),
        pltpu.VMEM((rows, DH), F32),
        pltpu.VMEM((rows, DH), F32),
        pltpu.VMEM((2 * tiles, rows, qw), BF16),
        pltpu.VMEM((2 * tiles, rows, qw), BF16),
        pltpu.VMEM((2 * tiles, rows, qw), BF16),
        pltpu.VMEM((2 * tiles, 2, rows, DH), BF16),
        pltpu.SemaphoreType.DMA((2 * tiles, 7)),
    ]
    flops = 2 * 5 * tiles * rows * GROUPS * span * DH
    outs = pl.pallas_call(
        functools.partial(head_kernel, head, offsets),
        in_specs=in_specs,
        out_specs=[hbm] * 4 + [vmem] * 2,
        scratch_shapes=scratch,
        out_shape=out_shape,
        input_output_aliases=aliases,
        cost_estimate=pl.CostEstimate(
            flops=flops, bytes_accessed=8 * tiles * rows * qw, transcendentals=0
        ),
        compiler_params=pltpu.CompilerParams(vmem_limit_bytes=32 * 2**20),
    )(*meta, *args)
    return list(outs[:4]), outs[4], outs[5]


def local(query, grad_out, branch_kv, root_kv, lengths, segments):
    n_dev = lax.axis_size("dev")
    n_grp = lax.axis_size("grp")
    me = lax.axis_index("dev")
    core = me % CORES
    _, _, qcols = query.shape
    kcols = root_kv.shape[1] // 2
    offsets = tuple(range(0, n_dev, 2 * CORES))

    def cols(x, which, parts):
        part = x.shape[-1] // parts
        wide = part // CORES
        axis = x.ndim - 1
        pieces = [
            lax.dynamic_slice_in_dim(x, p * part + which * wide, wide, axis) for p in range(parts)
        ]
        return pieces

    mine = cols(root_kv, core, 2)
    other = jnp.concatenate(cols(root_kv, 1 - core, 2), axis=1)
    got = swapped(other, "dev", 1)
    got = [got[:, : kcols // CORES], got[:, kcols // CORES :]]
    gathered = []
    for head in range(HEADS):
        at = slice(head * DH, (head + 1) * DH)
        x = jnp.stack(
            [
                jnp.concatenate([mine[0][:, at], mine[1][:, at]], axis=1),
                jnp.concatenate([got[0][:, at], got[1][:, at]], axis=1),
            ]
        )[None]
        arrived = [swapped(x, "dev", off) for off in offsets[1:]]
        x = jnp.concatenate([x] + arrived, axis=0)
        nxt = swapped(x, "dev", CORES)
        gathered.append((x, nxt))

    q_far = swapped(query, "dev", 1)
    g_far = swapped(grad_out, "dev", 1)
    b_far = swapped(branch_kv, "dev", 1)
    meta = (lengths, swapped(lengths, "dev", 1), segments, swapped(segments, "dev", 1))

    outs = None
    sums = []
    for head in range(HEADS):
        near, nxt = gathered[head]
        outs, keep, send = head_grads(
            head, offsets, meta, query, q_far, grad_out, g_far, branch_kv, b_far, near, nxt, outs
        )
        back = swapped(send, "dev", CORES)
        x = keep + back
        arrived = [swapped(x[j].astype(BF16), "dev", offsets[j]) for j in range(1, len(offsets))]
        x = x[0]
        for part in arrived:
            x = x + part
        sums.append(x)
    x = jnp.concatenate(
        [s[:, :, part * DH : (part + 1) * DH] for part in range(2) for s in sums], axis=2
    )
    hop = 1
    while hop < n_grp:
        x = x.astype(BF16)
        back = swapped(x, "grp", hop)
        x = x.astype(F32) + back.astype(F32)
        hop *= 2
    far = swapped(x[1], "dev", 1)
    near = x[0]
    wide = HEADS * DH
    pieces = []
    for part in range(2):
        at = slice(part * wide, (part + 1) * wide)
        for side in range(CORES):
            pieces.append(jnp.where(core == side, near[:, at], far[:, at]))
    root_grad = jnp.concatenate(pieces, axis=1)

    dq, dq_far, db, db_far = outs
    dq_got = swapped(dq_far, "dev", 1)
    db_got = swapped(db_far, "dev", 1)
    query_grad = lax.dynamic_update_slice_in_dim(dq, dq_got, (1 - core) * (qcols // CORES), 2)
    branch_grad = db
    for part in range(2):
        branch_grad = lax.dynamic_update_slice_in_dim(
            branch_grad,
            db_got[:, :, part * wide : (part + 1) * wide],
            (part * CORES + 1 - core) * wide,
            2,
        )
    return (query_grad, branch_grad, root_grad)


def solution(mesh):
    placed = (
        P(("grp", "dev"), None, None),
        P(("grp", "dev"), None, None),
        P(("grp", "dev"), None, None),
        P("dev", None),
        P(("grp", "dev")),
        P(("grp", "dev")),
    )

    return jax.shard_map(
        local,
        mesh=mesh,
        in_specs=placed,
        out_specs=(P(("grp", "dev"), None, None), P(("grp", "dev"), None, None), P("dev", None)),
        check_vma=False,
    )
```

```python
import functools
import math

import jax
import jax.numpy as jnp
from jax import lax
from jax.experimental import pallas as pl
from jax.experimental.pallas import tpu as pltpu
from jax.sharding import PartitionSpec as P


H = 32
KVH = 4
DH = 128
SEGS = 4
GROUPS = H // KVH
CORES = 2
HEADS = KVH // CORES
CHUNK = 32
BLOCK = 256
NT = (((1,), (1,)), ((), ()))
NN = (((1,), (0,)), ((), ()))
F32 = jnp.float32
BF16 = jnp.bfloat16


def swapped(block, axis, bit):
    route = [(i ^ bit, i) for i in range(lax.axis_size(axis))]
    return lax.ppermute(block, axis, route)


def dot(a, b, dims):
    return lax.dot_general(a, b, dims, preferred_element_type=F32)


def head_kernel(head, offsets, len_own, len_far, seg_own, seg_far, *refs):
    ins, refs = refs[:8], refs[-22:]
    q_own, q_far, g_own, g_far, b_own, b_far, kv_near, kv_next = ins
    dq_own, dq_far, db_own, db_far, keep, send = refs[:6]
    pairs, keys_t, bkeys, bvalues, bkeys_t, s_scr, dp_scr = refs[6:13]
    dk_acc, dv_acc, dbk_acc, dbv_acc, q_buf, g_buf, dq_buf, db_buf = refs[13:21]
    in_sem = refs[21]
    tiles, rows, _ = q_own.shape
    me = lax.axis_index("dev")
    core = me % CORES
    rr = kv_near.shape[2]
    roots = pairs.shape[0]
    width = roots // SEGS
    qw = GROUPS * DH
    scale = DH ** (-0.5)
    sharp = scale * math.log2(math.e)
    wide = pl.ds(pl.multiple_of((core * HEADS + head) * qw, qw), qw)
    narrow = pl.ds(pl.multiple_of((core * HEADS + head) * DH, DH), DH)
    v_narrow = pl.ds(pl.multiple_of((KVH + core * HEADS + head) * DH, DH), DH)

    def picked(t, near_ref, far_ref):
        near = near_ref[jnp.minimum(t, tiles - 1)]
        return jnp.where(t < tiles, near, far_ref[jnp.maximum(t - tiles, 0)])

    def places():
        n = 0
        for side in range(2):
            for j, off in enumerate(offsets):
                for b0 in range(CORES):
                    rel = b0 + side * CORES + off
                    yield n, side, j, b0, pl.multiple_of((me ^ rel) * rr, rr)
                    n += 1

    def tile_copies(t, out):
        if t < tiles:
            q_ref, g_ref, b_ref, dq_ref, db_ref = q_own, g_own, b_own, dq_own, db_own
            at, dq_at, db_at, dv_at = t, wide, narrow, v_narrow
        else:
            q_ref, g_ref, b_ref, dq_ref, db_ref = q_far, g_far, b_far, dq_far, db_far
            at, dq_at = t - tiles, pl.ds(head * qw, qw)
            db_at, dv_at = pl.ds(head * DH, DH), pl.ds((HEADS + head) * DH, DH)
        reads = (
            (q_ref.at[at, :, wide], q_buf.at[t]),
            (g_ref.at[at, :, wide], g_buf.at[t]),
            (b_ref.at[at, :, narrow], bkeys.at[t]),
            (b_ref.at[at, :, v_narrow], bvalues.at[t]),
        )
        writes = (
            (dq_buf.at[t], dq_ref.at[at, :, dq_at]),
            (db_buf.at[t, 0], db_ref.at[at, :, db_at]),
            (db_buf.at[t, 1], db_ref.at[at, :, dv_at]),
        )
        chosen = writes if out else reads
        return [
            pltpu.make_async_copy(src, dst, in_sem.at[t, i + (len(reads) if out else 0)])
            for i, (src, dst) in enumerate(chosen)
        ]

    for t in range(2 * tiles):

        @pl.when(picked(t, len_own, len_far) > 0)
        def _():
            for copy in tile_copies(t, False):
                copy.start()

    dk_acc[...] = jnp.zeros_like(dk_acc)
    dv_acc[...] = jnp.zeros_like(dv_acc)
    for _, side, j, b0, at in places():
        pairs[pl.ds(at, rr), :] = (kv_near, kv_next)[side][j, b0]
    for b in range(0, roots, DH):
        keys_t[:, b : b + DH] = pairs[b : b + DH, :DH].T

    def fold(x, op):
        return op(x.reshape(x.shape[0] // 8, 8, x.shape[1]), axis=0)

    def tile(t, carry):
        length = picked(t, len_own, len_far)
        segment = picked(t, seg_own, seg_far)

        dbk_acc[...] = jnp.zeros_like(dbk_acc)
        dbv_acc[...] = jnp.zeros_like(dbv_acc)

        for at in range(2 * tiles):

            @pl.when((t == at) & (length > 0))
            def _():
                for copy in tile_copies(at, False):
                    copy.wait()

        bkeys_t[...] = bkeys[t].T

        def pieces(starts, segs):
            size = CHUNK
            qrows = GROUPS * size
            every = range(len(starts))
            lanes = [slice(i * qrows, (i + 1) * qrows) for i in every]
            count = segs * width // BLOCK
            spans = [(b * BLOCK, BLOCK) for b in range(count)] + [(roots, rows)]
            ats = [slice(lo, lo + n) for lo, n in spans]

            def stacked(ref, r0):
                x = ref[t, pl.ds(r0, size), :]
                return jnp.concatenate([x[:, j * DH : (j + 1) * DH] for j in range(GROUPS)], axis=0)

            def masked(g, r0):
                row = lax.broadcasted_iota(jnp.int32, (qrows, DH), 0) % size + r0
                return jnp.where(row < length, g.astype(F32), 0.0).astype(BF16)

            q = [stacked(q_buf, r0) for r0 in starts]
            g = [masked(stacked(g_buf, r0), r0) for r0 in starts]

            def k_of(b):
                return pairs[ats[b], :DH] if b < count else bkeys[t]

            def v_of(b):
                return pairs[ats[b], DH:] if b < count else bvalues[t]

            def kt_of(b):
                return keys_t[:, ats[b]] if b < count else bkeys_t[...]

            peaks, invs = [], []
            for i in every:
                top = None
                for b in range(count + 1):
                    s = dot(k_of(b), q[i], NT)
                    if b == count:
                        key = lax.broadcasted_iota(jnp.int32, s.shape, 0)
                        pos = lax.broadcasted_iota(jnp.int32, s.shape, 1) % size + starts[i]
                        s = jnp.where(key <= pos, s, F32(-1e30))
                    s_scr[ats[b], lanes[i]] = s
                    part = fold(s, jnp.max)
                    top = part if top is None else jnp.maximum(top, part)
                peaks.append(jnp.max(top, axis=0, keepdims=True))

            for i in every:
                total = jnp.zeros((8, qrows), F32)
                for b in range(count + 1):
                    dp_scr[ats[b], lanes[i]] = dot(v_of(b), g[i], NT)
                    e = jnp.exp2((s_scr[ats[b], lanes[i]] - peaks[i]) * sharp)
                    s_scr[ats[b], lanes[i]] = e
                    total = total + fold(e, jnp.sum)
                invs.append(1.0 / jnp.sum(total, axis=0, keepdims=True))

            deltas = []
            for i in every:
                delta = jnp.zeros((8, qrows), F32)
                for b in range(count + 1):
                    probs = (s_scr[ats[b], lanes[i]] * invs[i]).astype(BF16)
                    delta = delta + fold(probs.astype(F32) * dp_scr[ats[b], lanes[i]], jnp.sum)
                    dv = dot(probs, g[i], NN)
                    if b < count:
                        dv_acc[ats[b], :] += dv
                    else:
                        dbv_acc[...] += dv
                deltas.append(jnp.sum(delta, axis=0, keepdims=True))

            for i in every:
                dq_t = jnp.zeros((DH, qrows), F32)
                scaled = invs[i] * scale
                for b in range(count + 1):
                    ds = (s_scr[ats[b], lanes[i]] * scaled) * (dp_scr[ats[b], lanes[i]] - deltas[i])
                    ds = ds.astype(BF16)
                    dk = dot(ds, q[i], NN)
                    if b < count:
                        dk_acc[ats[b], :] += dk
                    else:
                        dbk_acc[...] += dk
                    dq_t = dq_t + dot(kt_of(b), ds, NN)
                dq = dq_t.T.astype(BF16)
                for j in range(GROUPS):
                    part = dq[j * size : (j + 1) * size, :]
                    dq_buf[t, pl.ds(starts[i], size), j * DH : (j + 1) * DH] = part

        count = (length + (CHUNK - 1)) // CHUNK
        for s in range(SEGS):

            @pl.when(segment == s)
            def _():
                def step(c, carry):
                    first = c * (2 * CHUNK)
                    pieces([pl.multiple_of(first + i * CHUNK, CHUNK) for i in range(2)], s + 1)
                    return carry

                lax.fori_loop(0, count // 2, step, 0)

                @pl.when(count % 2 == 1)
                def _():
                    pieces([pl.multiple_of((count - 1) * CHUNK, CHUNK)], s + 1)

        def clear(c, carry):
            at = pl.multiple_of(c * CHUNK, CHUNK)
            dq_buf[t, pl.ds(at, CHUNK), :] = jnp.zeros((CHUNK, qw), BF16)
            return carry

        lax.fori_loop(count, rows // CHUNK, clear, 0)
        db_buf[t, 0] = dbk_acc[...].astype(BF16)
        db_buf[t, 1] = dbv_acc[...].astype(BF16)
        for at in range(2 * tiles):

            @pl.when(t == at)
            def _():
                for copy in tile_copies(at, True):
                    copy.start()

        return carry

    lax.fori_loop(0, 2 * tiles, tile, 0)

    for _, side, j, b0, at in places():
        out = (keep, send)[side]
        out[j, b0, :, :DH] = dk_acc[pl.ds(at, rr), :].astype(out.dtype)
        out[j, b0, :, DH:] = dv_acc[pl.ds(at, rr), :].astype(out.dtype)
    for t in range(2 * tiles):
        for copy in tile_copies(t, True):
            copy.wait()


def head_grads(head, offsets, meta, q, q_far, g, g_far, b, b_far, near, nxt, earlier):
    tiles, rows, _ = q.shape
    half = near.shape[0]
    rr = near.shape[2]
    roots = 2 * half * CORES * rr
    qw = GROUPS * DH
    span = roots + rows
    vmem = pl.BlockSpec(memory_space=pltpu.VMEM)
    hbm = pl.BlockSpec(memory_space=pltpu.HBM)
    q, g, b = (pltpu.with_memory_space_constraint(x, pltpu.HBM) for x in (q, g, b))
    args = [q, q_far, g, g_far, b, b_far, near, nxt]
    in_specs = [pl.BlockSpec(memory_space=pltpu.SMEM)] * len(meta) + [hbm] * 6 + [vmem] * 2
    aliases = {}
    if earlier is not None:
        in_specs += [hbm] * 4
        aliases = {len(meta) + len(args) + i: i for i in range(4)}
        args += earlier
    out_shape = [
        jax.ShapeDtypeStruct(q.shape, BF16),
        jax.ShapeDtypeStruct((tiles, rows, HEADS * qw), BF16),
        jax.ShapeDtypeStruct(b.shape, BF16),
        jax.ShapeDtypeStruct((tiles, rows, 2 * HEADS * DH), BF16),
        jax.ShapeDtypeStruct(near.shape, F32),
        jax.ShapeDtypeStruct(near.shape, BF16),
    ]
    scratch = [
        pltpu.VMEM((roots, 2 * DH), BF16),
        pltpu.VMEM((DH, roots), BF16),
        pltpu.VMEM((2 * tiles, rows, DH), BF16),
        pltpu.VMEM((2 * tiles, rows, DH), BF16),
        pltpu.VMEM((DH, rows), BF16),
        pltpu.VMEM((span, 2 * CHUNK * GROUPS), F32),
        pltpu.VMEM((span, 2 * CHUNK * GROUPS), F32),
        pltpu.VMEM((roots, DH), F32),
        pltpu.VMEM((roots, DH), F32),
        pltpu.VMEM((rows, DH), F32),
        pltpu.VMEM((rows, DH), F32),
        pltpu.VMEM((2 * tiles, rows, qw), BF16),
        pltpu.VMEM((2 * tiles, rows, qw), BF16),
        pltpu.VMEM((2 * tiles, rows, qw), BF16),
        pltpu.VMEM((2 * tiles, 2, rows, DH), BF16),
        pltpu.SemaphoreType.DMA((2 * tiles, 7)),
    ]
    flops = 2 * 5 * tiles * rows * GROUPS * span * DH
    outs = pl.pallas_call(
        functools.partial(head_kernel, head, offsets),
        in_specs=in_specs,
        out_specs=[hbm] * 4 + [vmem] * 2,
        scratch_shapes=scratch,
        out_shape=out_shape,
        input_output_aliases=aliases,
        cost_estimate=pl.CostEstimate(
            flops=flops, bytes_accessed=8 * tiles * rows * qw, transcendentals=0
        ),
        compiler_params=pltpu.CompilerParams(vmem_limit_bytes=32 * 2**20),
    )(*meta, *args)
    return list(outs[:4]), outs[4], outs[5]


def local(query, grad_out, branch_kv, root_kv, lengths, segments):
    n_dev = lax.axis_size("dev")
    n_grp = lax.axis_size("grp")
    me = lax.axis_index("dev")
    core = me % CORES
    _, _, qcols = query.shape
    kcols = root_kv.shape[1] // 2
    offsets = tuple(range(0, n_dev, 2 * CORES))

    def cols(x, which, parts):
        part = x.shape[-1] // parts
        wide = part // CORES
        axis = x.ndim - 1
        pieces = [
            lax.dynamic_slice_in_dim(x, p * part + which * wide, wide, axis) for p in range(parts)
        ]
        return pieces

    mine = cols(root_kv, core, 2)
    other = jnp.concatenate(cols(root_kv, 1 - core, 2), axis=1)
    got = swapped(other, "dev", 1)
    got = [got[:, : kcols // CORES], got[:, kcols // CORES :]]
    gathered = []
    for head in range(HEADS):
        at = slice(head * DH, (head + 1) * DH)
        x = jnp.stack(
            [
                jnp.concatenate([mine[0][:, at], mine[1][:, at]], axis=1),
                jnp.concatenate([got[0][:, at], got[1][:, at]], axis=1),
            ]
        )[None]
        arrived = []
        for off in offsets[1:]:
            arrived.append(swapped(x, "dev", off))
        x = jnp.concatenate([x] + arrived, axis=0)
        nxt = swapped(x, "dev", CORES)
        gathered.append((x, nxt))

    q_far = swapped(query, "dev", 1)
    g_far = swapped(grad_out, "dev", 1)
    b_far = swapped(branch_kv, "dev", 1)
    meta = (lengths, swapped(lengths, "dev", 1), segments, swapped(segments, "dev", 1))

    outs = None
    sums = []
    for head in range(HEADS):
        near, nxt = gathered[head]
        outs, keep, send = head_grads(
            head, offsets, meta, query, q_far, grad_out, g_far, branch_kv, b_far, near, nxt, outs
        )
        back = swapped(send, "dev", CORES)
        x = keep + back
        arrived = []
        for j in range(1, len(offsets)):
            arrived.append(swapped(x[j].astype(BF16), "dev", offsets[j]))
        x = x[0]
        for part in arrived:
            x = x + part
        hop = 1
        while hop < n_grp:
            x = x.astype(BF16)
            back = swapped(x, "grp", hop)
            x = x.astype(F32) + back.astype(F32)
            hop *= 2
        sums.append(x)
    x = jnp.concatenate(
        [s[:, :, part * DH : (part + 1) * DH] for part in range(2) for s in sums], axis=2
    )
    far = swapped(x[1], "dev", 1)
    near = x[0]
    wide = HEADS * DH
    pieces = []
    for part in range(2):
        at = slice(part * wide, (part + 1) * wide)
        for side in range(CORES):
            pieces.append(jnp.where(core == side, near[:, at], far[:, at]))
    root_grad = jnp.concatenate(pieces, axis=1)

    dq, dq_far, db, db_far = outs
    dq_got = swapped(dq_far, "dev", 1)
    db_got = swapped(db_far, "dev", 1)
    query_grad = lax.dynamic_update_slice_in_dim(dq, dq_got, (1 - core) * (qcols // CORES), 2)
    branch_grad = db
    for part in range(2):
        branch_grad = lax.dynamic_update_slice_in_dim(
            branch_grad,
            db_got[:, :, part * wide : (part + 1) * wide],
            (part * CORES + 1 - core) * wide,
            2,
        )
    return (query_grad, branch_grad, root_grad)


def solution(mesh):
    placed = (
        P(("grp", "dev"), None, None),
        P(("grp", "dev"), None, None),
        P(("grp", "dev"), None, None),
        P("dev", None),
        P(("grp", "dev")),
        P(("grp", "dev")),
    )

    return jax.shard_map(
        local,
        mesh=mesh,
        in_specs=placed,
        out_specs=(P(("grp", "dev"), None, None), P(("grp", "dev"), None, None), P("dev", None)),
        check_vma=False,
    )
```

```python
import functools
import math

import jax
import jax.numpy as jnp
from jax import lax
from jax.experimental import pallas as pl
from jax.experimental.pallas import tpu as pltpu
from jax.sharding import PartitionSpec as P


H = 32
KVH = 4
DH = 128
SEGS = 4
GROUPS = H // KVH
CORES = 2
HEADS = KVH // CORES
CHUNK = 32
BLOCK = 256
NT = (((1,), (1,)), ((), ()))
NN = (((1,), (0,)), ((), ()))
F32 = jnp.float32
BF16 = jnp.bfloat16


def swapped(block, axis, bit):
    route = [(i ^ bit, i) for i in range(lax.axis_size(axis))]
    return lax.ppermute(block, axis, route)


def dot(a, b, dims):
    return lax.dot_general(a, b, dims, preferred_element_type=F32)


def head_kernel(head, offsets, len_own, len_far, seg_own, seg_far, *refs):
    ins, refs = refs[:8], refs[-22:]
    q_own, q_far, g_own, g_far, b_own, b_far, kv_near, kv_next = ins
    dq_own, dq_far, db_own, db_far, keep, send = refs[:6]
    pairs, keys_t, bkeys, bvalues, bkeys_t, s_scr, dp_scr = refs[6:13]
    dk_acc, dv_acc, dbk_acc, dbv_acc, q_buf, g_buf, dq_buf, db_buf = refs[13:21]
    in_sem = refs[21]
    tiles, rows, _ = q_own.shape
    me = lax.axis_index("dev")
    core = me % CORES
    rr = kv_near.shape[2]
    roots = pairs.shape[0]
    width = roots // SEGS
    qw = GROUPS * DH
    scale = DH ** (-0.5)
    sharp = scale * math.log2(math.e)
    wide = pl.ds(pl.multiple_of((core * HEADS + head) * qw, qw), qw)
    narrow = pl.ds(pl.multiple_of((core * HEADS + head) * DH, DH), DH)
    v_narrow = pl.ds(pl.multiple_of((KVH + core * HEADS + head) * DH, DH), DH)

    def picked(t, near_ref, far_ref):
        near = near_ref[jnp.minimum(t, tiles - 1)]
        return jnp.where(t < tiles, near, far_ref[jnp.maximum(t - tiles, 0)])

    def places():
        n = 0
        for side in range(2):
            for j, off in enumerate(offsets):
                for b0 in range(CORES):
                    rel = b0 + side * CORES + off
                    yield n, side, j, b0, pl.multiple_of((me ^ rel) * rr, rr)
                    n += 1

    def tile_copies(t, out):
        if t < tiles:
            q_ref, g_ref, b_ref, dq_ref, db_ref = q_own, g_own, b_own, dq_own, db_own
            at, dq_at, db_at, dv_at = t, wide, narrow, v_narrow
        else:
            q_ref, g_ref, b_ref, dq_ref, db_ref = q_far, g_far, b_far, dq_far, db_far
            at, dq_at = t - tiles, pl.ds(head * qw, qw)
            db_at, dv_at = pl.ds(head * DH, DH), pl.ds((HEADS + head) * DH, DH)
        reads = (
            (q_ref.at[at, :, wide], q_buf.at[t]),
            (g_ref.at[at, :, wide], g_buf.at[t]),
            (b_ref.at[at, :, narrow], bkeys.at[t]),
            (b_ref.at[at, :, v_narrow], bvalues.at[t]),
        )
        writes = (
            (dq_buf.at[t], dq_ref.at[at, :, dq_at]),
            (db_buf.at[t, 0], db_ref.at[at, :, db_at]),
            (db_buf.at[t, 1], db_ref.at[at, :, dv_at]),
        )
        chosen = writes if out else reads
        return [
            pltpu.make_async_copy(src, dst, in_sem.at[t, i + (len(reads) if out else 0)])
            for i, (src, dst) in enumerate(chosen)
        ]

    for t in range(2 * tiles):

        @pl.when(picked(t, len_own, len_far) > 0)
        def _():
            for copy in tile_copies(t, False):
                copy.start()

    dk_acc[...] = jnp.zeros_like(dk_acc)
    dv_acc[...] = jnp.zeros_like(dv_acc)
    for _, side, j, b0, at in places():
        pairs[pl.ds(at, rr), :] = (kv_near, kv_next)[side][j, b0]
    for b in range(0, roots, DH):
        keys_t[:, b : b + DH] = pairs[b : b + DH, :DH].T

    def fold(x, op):
        return op(x.reshape(x.shape[0] // 8, 8, x.shape[1]), axis=0)

    def tile(t, carry):
        length = picked(t, len_own, len_far)
        segment = picked(t, seg_own, seg_far)

        dbk_acc[...] = jnp.zeros_like(dbk_acc)
        dbv_acc[...] = jnp.zeros_like(dbv_acc)

        for at in range(2 * tiles):

            @pl.when((t == at) & (length > 0))
            def _():
                for copy in tile_copies(at, False):
                    copy.wait()

        bkeys_t[...] = bkeys[t].T

        def pieces(starts, seen, segs):
            size = CHUNK
            qrows = GROUPS * size
            every = range(len(starts))
            lanes = [slice(i * qrows, (i + 1) * qrows) for i in every]
            count = segs * width // BLOCK
            ats = [slice(b * BLOCK, (b + 1) * BLOCK) for b in range(count)]

            def stacked(ref, r0):
                x = ref[t, pl.ds(r0, size), :]
                return jnp.concatenate([x[:, j * DH : (j + 1) * DH] for j in range(GROUPS)], axis=0)

            def masked(g, r0):
                row = lax.broadcasted_iota(jnp.int32, (qrows, DH), 0) % size + r0
                return jnp.where(row < length, g.astype(F32), 0.0).astype(BF16)

            q = [stacked(q_buf, r0) for r0 in starts]
            g = [masked(stacked(g_buf, r0), r0) for r0 in starts]

            def at_of(i, b):
                return ats[b] if b < count else slice(roots, roots + seen[i])

            def k_of(i, b):
                return pairs[ats[b], :DH] if b < count else bkeys[t, : seen[i], :]

            def v_of(i, b):
                return pairs[ats[b], DH:] if b < count else bvalues[t, : seen[i], :]

            def kt_of(i, b):
                return keys_t[:, ats[b]] if b < count else bkeys_t[:, : seen[i]]

            peaks, invs = [], []
            for i in every:
                top = None
                for b in range(count + 1):
                    s = dot(k_of(i, b), q[i], NT)
                    if b == count:
                        key = lax.broadcasted_iota(jnp.int32, s.shape, 0)
                        pos = lax.broadcasted_iota(jnp.int32, s.shape, 1) % size + starts[i]
                        s = jnp.where(key <= pos, s, F32(-1e30))
                    s_scr[at_of(i, b), lanes[i]] = s
                    part = fold(s, jnp.max)
                    top = part if top is None else jnp.maximum(top, part)
                peaks.append(jnp.max(top, axis=0, keepdims=True))

            for i in every:
                total = jnp.zeros((8, qrows), F32)
                for b in range(count + 1):
                    dp_scr[at_of(i, b), lanes[i]] = dot(v_of(i, b), g[i], NT)
                    e = jnp.exp2((s_scr[at_of(i, b), lanes[i]] - peaks[i]) * sharp)
                    s_scr[at_of(i, b), lanes[i]] = e
                    total = total + fold(e, jnp.sum)
                invs.append(1.0 / jnp.sum(total, axis=0, keepdims=True))

            deltas = []
            for i in every:
                delta = jnp.zeros((8, qrows), F32)
                for b in range(count + 1):
                    probs = (s_scr[at_of(i, b), lanes[i]] * invs[i]).astype(BF16)
                    delta = delta + fold(probs.astype(F32) * dp_scr[at_of(i, b), lanes[i]], jnp.sum)
                    dv = dot(probs, g[i], NN)
                    if b < count:
                        dv_acc[ats[b], :] += dv
                    else:
                        dbv_acc[: seen[i], :] += dv
                deltas.append(jnp.sum(delta, axis=0, keepdims=True))

            for i in every:
                dq_t = jnp.zeros((DH, qrows), F32)
                scaled = invs[i] * scale
                for b in range(count + 1):
                    ds = (s_scr[at_of(i, b), lanes[i]] * scaled) * (dp_scr[at_of(i, b), lanes[i]] - deltas[i])
                    ds = ds.astype(BF16)
                    dk = dot(ds, q[i], NN)
                    if b < count:
                        dk_acc[ats[b], :] += dk
                    else:
                        dbk_acc[: seen[i], :] += dk
                    dq_t = dq_t + dot(kt_of(i, b), ds, NN)
                dq = dq_t.T.astype(BF16)
                for j in range(GROUPS):
                    part = dq[j * size : (j + 1) * size, :]
                    dq_buf[t, pl.ds(starts[i], size), j * DH : (j + 1) * DH] = part

        count = (length + (CHUNK - 1)) // CHUNK
        for s in range(SEGS):

            @pl.when(segment == s)
            def _():
                for pair in range(rows // (2 * CHUNK)):

                    @pl.when(pair < count // 2)
                    def _():
                        first = [(2 * pair + i) * CHUNK for i in range(2)]
                        pieces(first, [r0 + CHUNK for r0 in first], s + 1)

                @pl.when(count % 2 == 1)
                def _():
                    at = pl.multiple_of((count - 1) * CHUNK, CHUNK)
                    pieces([at], [rows - CHUNK], s + 1)

        def clear(c, carry):
            at = pl.multiple_of(c * CHUNK, CHUNK)
            dq_buf[t, pl.ds(at, CHUNK), :] = jnp.zeros((CHUNK, qw), BF16)
            return carry

        lax.fori_loop(count, rows // CHUNK, clear, 0)
        db_buf[t, 0] = dbk_acc[...].astype(BF16)
        db_buf[t, 1] = dbv_acc[...].astype(BF16)
        for at in range(2 * tiles):

            @pl.when(t == at)
            def _():
                for copy in tile_copies(at, True):
                    copy.start()

        return carry

    lax.fori_loop(0, 2 * tiles, tile, 0)

    for _, side, j, b0, at in places():
        out = (keep, send)[side]
        out[j, b0, :, :DH] = dk_acc[pl.ds(at, rr), :].astype(out.dtype)
        out[j, b0, :, DH:] = dv_acc[pl.ds(at, rr), :].astype(out.dtype)
    for t in range(2 * tiles):
        for copy in tile_copies(t, True):
            copy.wait()


def head_grads(head, offsets, meta, q, q_far, g, g_far, b, b_far, near, nxt, earlier):
    tiles, rows, _ = q.shape
    half = near.shape[0]
    rr = near.shape[2]
    roots = 2 * half * CORES * rr
    qw = GROUPS * DH
    span = roots + rows
    vmem = pl.BlockSpec(memory_space=pltpu.VMEM)
    hbm = pl.BlockSpec(memory_space=pltpu.HBM)
    q, g, b = (pltpu.with_memory_space_constraint(x, pltpu.HBM) for x in (q, g, b))
    args = [q, q_far, g, g_far, b, b_far, near, nxt]
    in_specs = [pl.BlockSpec(memory_space=pltpu.SMEM)] * len(meta) + [hbm] * 6 + [vmem] * 2
    aliases = {}
    if earlier is not None:
        in_specs += [hbm] * 4
        aliases = {len(meta) + len(args) + i: i for i in range(4)}
        args += earlier
    out_shape = [
        jax.ShapeDtypeStruct(q.shape, BF16),
        jax.ShapeDtypeStruct((tiles, rows, HEADS * qw), BF16),
        jax.ShapeDtypeStruct(b.shape, BF16),
        jax.ShapeDtypeStruct((tiles, rows, 2 * HEADS * DH), BF16),
        jax.ShapeDtypeStruct(near.shape, F32),
        jax.ShapeDtypeStruct(near.shape, BF16),
    ]
    scratch = [
        pltpu.VMEM((roots, 2 * DH), BF16),
        pltpu.VMEM((DH, roots), BF16),
        pltpu.VMEM((2 * tiles, rows, DH), BF16),
        pltpu.VMEM((2 * tiles, rows, DH), BF16),
        pltpu.VMEM((DH, rows), BF16),
        pltpu.VMEM((span, 2 * CHUNK * GROUPS), F32),
        pltpu.VMEM((span, 2 * CHUNK * GROUPS), F32),
        pltpu.VMEM((roots, DH), F32),
        pltpu.VMEM((roots, DH), F32),
        pltpu.VMEM((rows, DH), F32),
        pltpu.VMEM((rows, DH), F32),
        pltpu.VMEM((2 * tiles, rows, qw), BF16),
        pltpu.VMEM((2 * tiles, rows, qw), BF16),
        pltpu.VMEM((2 * tiles, rows, qw), BF16),
        pltpu.VMEM((2 * tiles, 2, rows, DH), BF16),
        pltpu.SemaphoreType.DMA((2 * tiles, 7)),
    ]
    flops = 2 * 5 * tiles * rows * GROUPS * span * DH
    outs = pl.pallas_call(
        functools.partial(head_kernel, head, offsets),
        in_specs=in_specs,
        out_specs=[hbm] * 4 + [vmem] * 2,
        scratch_shapes=scratch,
        out_shape=out_shape,
        input_output_aliases=aliases,
        cost_estimate=pl.CostEstimate(
            flops=flops, bytes_accessed=8 * tiles * rows * qw, transcendentals=0
        ),
        compiler_params=pltpu.CompilerParams(vmem_limit_bytes=32 * 2**20),
    )(*meta, *args)
    return list(outs[:4]), outs[4], outs[5]


def local(query, grad_out, branch_kv, root_kv, lengths, segments):
    n_dev = lax.axis_size("dev")
    n_grp = lax.axis_size("grp")
    me = lax.axis_index("dev")
    core = me % CORES
    _, _, qcols = query.shape
    kcols = root_kv.shape[1] // 2
    offsets = tuple(range(0, n_dev, 2 * CORES))

    def cols(x, which, parts):
        part = x.shape[-1] // parts
        wide = part // CORES
        axis = x.ndim - 1
        pieces = [
            lax.dynamic_slice_in_dim(x, p * part + which * wide, wide, axis) for p in range(parts)
        ]
        return pieces

    mine = cols(root_kv, core, 2)
    other = jnp.concatenate(cols(root_kv, 1 - core, 2), axis=1)
    got = swapped(other, "dev", 1)
    got = [got[:, : kcols // CORES], got[:, kcols // CORES :]]
    gathered = []
    for head in range(HEADS):
        at = slice(head * DH, (head + 1) * DH)
        x = jnp.stack(
            [
                jnp.concatenate([mine[0][:, at], mine[1][:, at]], axis=1),
                jnp.concatenate([got[0][:, at], got[1][:, at]], axis=1),
            ]
        )[None]
        arrived = []
        for off in offsets[1:]:
            arrived.append(swapped(x, "dev", off))
        x = jnp.concatenate([x] + arrived, axis=0)
        nxt = swapped(x, "dev", CORES)
        gathered.append((x, nxt))

    q_far = swapped(query, "dev", 1)
    g_far = swapped(grad_out, "dev", 1)
    b_far = swapped(branch_kv, "dev", 1)
    meta = (lengths, swapped(lengths, "dev", 1), segments, swapped(segments, "dev", 1))

    outs = None
    sums = []
    for head in range(HEADS):
        near, nxt = gathered[head]
        outs, keep, send = head_grads(
            head, offsets, meta, query, q_far, grad_out, g_far, branch_kv, b_far, near, nxt, outs
        )
        back = swapped(send, "dev", CORES)
        x = keep + back
        arrived = []
        for j in range(1, len(offsets)):
            arrived.append(swapped(x[j].astype(BF16), "dev", offsets[j]))
        x = x[0]
        for part in arrived:
            x = x + part
        hop = 1
        while hop < n_grp:
            x = x.astype(BF16)
            back = swapped(x, "grp", hop)
            x = x.astype(F32) + back.astype(F32)
            hop *= 2
        sums.append(x)
    x = jnp.concatenate(
        [s[:, :, part * DH : (part + 1) * DH] for part in range(2) for s in sums], axis=2
    )
    far = swapped(x[1], "dev", 1)
    near = x[0]
    wide = HEADS * DH
    pieces = []
    for part in range(2):
        at = slice(part * wide, (part + 1) * wide)
        for side in range(CORES):
            pieces.append(jnp.where(core == side, near[:, at], far[:, at]))
    root_grad = jnp.concatenate(pieces, axis=1)

    dq, dq_far, db, db_far = outs
    dq_got = swapped(dq_far, "dev", 1)
    db_got = swapped(db_far, "dev", 1)
    query_grad = lax.dynamic_update_slice_in_dim(dq, dq_got, (1 - core) * (qcols // CORES), 2)
    branch_grad = db
    for part in range(2):
        branch_grad = lax.dynamic_update_slice_in_dim(
            branch_grad,
            db_got[:, :, part * wide : (part + 1) * wide],
            (part * CORES + 1 - core) * wide,
            2,
        )
    return (query_grad, branch_grad, root_grad)


def solution(mesh):
    placed = (
        P(("grp", "dev"), None, None),
        P(("grp", "dev"), None, None),
        P(("grp", "dev"), None, None),
        P("dev", None),
        P(("grp", "dev")),
        P(("grp", "dev")),
    )

    return jax.shard_map(
        local,
        mesh=mesh,
        in_specs=placed,
        out_specs=(P(("grp", "dev"), None, None), P(("grp", "dev"), None, None), P("dev", None)),
        check_vma=False,
    )
```
